128 devices in a mesh: elem: 128 (over x, y, z, core).
Axes of the slice: x: 4, y: 4, z: 4, core: 2. Of those that a mesh axis runs over, the one named last changes fastest.
Arguments:
- tracer: float32 [1024, 8, 640], P('elem'), may hold values from 0 to 1
- old_mass: float32 [1024, 128], P('elem'), may hold values from 0.3 to 3
- new_mass: float32 [1024, 128], P('elem'), may hold values from 0.3 to 3
- dep_owner: int32 [1024, 128, 1], P('elem'), may hold values from 0 to 127, as said below
- dep_local: int32 [1024, 128], P('elem'), may hold values from 0 to 7
- dep_coord: float32 [2, 1024, 128], P(None, 'elem'), may hold values from -1 to 1
Outputs:
- new_tracer: float32 [1024, 8, 640], P('elem')
The draws below stay inside these ranges and needn't reach their ends.
Inputs may be any that keep to these rules, and one draw needn't show every extreme that they name: `dep_owner`: the rows of one device name their own device or one of at most five other devices; no other device is named more than 32 times among them, and one other device is named exactly 32 times.
All inputs are finite; a program needn't handle non-finite values.
Results may differ from the reference program's by a relative error of at most 0.0003.
Values sent between devices are 32-bit elements; how exact they have to be, the bound alone decides.
No kernel may reach another device: no remote copies, remote signals or barrier semaphores. Data moves between devices by JAX's collectives and lax.ppermute only.
A program may use at most 64 MiB of HBM per device.

```python
import math
import jax
import jax.numpy as jnp
from jax import lax

E_DEV = 8
LEV = 8
NP2 = 16
Q = 40
ELEMS = 1024
N_ELEM = 128


def draw_dep_owner(key, part):
    rows = E_DEV * LEV * NP2
    bound = rows // 32
    keys = jax.random.split(jax.random.fold_in(key, 7031), N_ELEM)
    devices = jnp.arange(N_ELEM, dtype=jnp.int32)

    def one_device(dev_key, device):
        key_count, key_pick, key_perm, key_peer = jax.random.split(dev_key, 4)
        shuffled = jax.random.permutation(key_peer, N_ELEM - 1).astype(jnp.int32) + 1
        offsets = shuffled[:5]
        counts = jax.random.randint(key_count, (5,), max(1, bound // 4), bound + 1, dtype=jnp.int32)
        pick = jax.random.randint(key_pick, (), 0, 5, dtype=jnp.int32)
        counts = jnp.where(jnp.arange(5, dtype=jnp.int32) == pick, bound, counts)
        limits = jnp.cumsum(counts)
        position = jnp.arange(rows, dtype=jnp.int32)
        which = jnp.sum((position[:, None] >= limits[None, :]).astype(jnp.int32), axis=1)
        neighbour = (device + offsets[jnp.minimum(which, 4)]) % N_ELEM
        owners = jnp.where(which < 5, neighbour, device).astype(jnp.int32)
        order = jax.random.permutation(key_perm, rows)
        return owners[order]
    owners = jax.vmap(one_device)(keys, devices)
    return owners.reshape(N_ELEM * E_DEV, LEV * NP2, 1).astype(jnp.int32)


def plant(drawn, rng, least, top_value):
    longest = drawn.shape.index(max(drawn.shape))
    spots = []
    for shift in (0, 1):
        where = [jax.random.randint(jax.random.fold_in(rng, axis), (), 0, length) for axis, length in enumerate(drawn.shape)]
        where[longest] = (where[longest] + shift) % drawn.shape[longest]
        spots.append(tuple(where))
    return drawn.at[spots[0]].set(least).at[spots[1]].set(top_value)


def shard_levels(rng, shape, cuts, least, top_value):
    gain, own = 1.0, jax.random.fold_in(rng, 6)
    for dim, parts in cuts:
        steps = jnp.exp(jax.random.uniform(jax.random.fold_in(own, dim), (parts,), jnp.float32, least / len(cuts), top_value / len(cuts)))
        gain = gain * jnp.repeat(steps, shape[dim] // parts).reshape([-1 if axis == dim else 1 for axis in range(len(shape))])
    return gain


def setup_inputs(seed: int = 0) -> dict:
    key_list = jax.random.split(jax.random.key(seed), 7)
    return {
        "tracer": jnp.clip(1.0 * jax.random.uniform(key_list[0], (ELEMS, LEV, NP2 * Q), jnp.float32) ** shard_levels(key_list[0], (ELEMS, LEV, NP2 * Q), ((0, 128),), -0.2, 0.2), 0.0, 1.0),
        "old_mass": jnp.clip(jnp.exp(math.log(3.0) - 2.3025851 * jax.random.uniform(key_list[1], (ELEMS, LEV * NP2), jnp.float32) ** shard_levels(key_list[1], (ELEMS, LEV * NP2), ((0, 128),), -0.2, 0.2)), 0.3, 3.0),
        "new_mass": jnp.clip(jnp.exp(math.log(3.0) - 2.3025851 * jax.random.uniform(key_list[2], (ELEMS, LEV * NP2), jnp.float32) ** shard_levels(key_list[2], (ELEMS, LEV * NP2), ((0, 128),), -0.2, 0.2)), 0.3, 3.0),
        "dep_owner": draw_dep_owner(jax.random.fold_in(key_list[6], 71), 0),
        "dep_local": plant(jax.random.randint(key_list[4], (ELEMS, LEV * NP2), 0, E_DEV), jax.random.fold_in(key_list[4], 1), 0, E_DEV - 1).astype(jnp.int32),
        "dep_coord": jnp.clip(jax.random.uniform(key_list[5], (2, ELEMS, LEV * NP2), jnp.float32, -1.0, 1.0) * shard_levels(key_list[5], (2, ELEMS, LEV * NP2), ((1, 128),), -0.4, 0.0), -1.0, 1.0),
    }


GLL_NODES = (-1.0, -0.4472135954999579, 0.4472135954999579, 1.0)


def one_axis(coord):
    columns = []
    for node_own in range(4):
        factor = jnp.ones_like(coord)
        for node_other in range(4):
            if node_other != node_own:
                factor = factor * (coord - GLL_NODES[node_other]) / (GLL_NODES[node_own] - GLL_NODES[node_other])
        columns.append(factor)
    return jnp.stack(columns, axis=-1)


def lagrange_weights(coord_a, coord_b):
    weights_a = one_axis(coord_a)
    weights_b = one_axis(coord_b)
    return (weights_a[..., :, None] * weights_b[..., None, :]).reshape(coord_a.shape + (16,))


def fixer_terms(interp, lowest, highest, mass_new):
    clipped = jnp.clip(interp, lowest, highest)
    margin = 0.01 + 0.05 * (highest - lowest)
    upper = highest + margin - clipped
    lower = clipped - lowest + margin
    sums = (jnp.sum(mass_new * clipped, axis=(0, 2)), jnp.sum(mass_new * upper, axis=(0, 2)), jnp.sum(mass_new * lower, axis=(0, 2)))
    return clipped, upper, lower, sums


def apply_fix(clipped, upper, lower, source_total, clip_total, up_total, down_total):
    deficit = (source_total - clip_total)[:, None, :]
    return clipped + jnp.maximum(deficit, 0.0) / up_total[:, None, :] * upper + jnp.minimum(deficit, 0.0) / down_total[:, None, :] * lower


def reference(tracer, old_mass, new_mass, dep_owner, dep_local, dep_coord):
    elems, levels, width = tracer.shape
    tracers = width // NP2
    table = tracer.reshape(elems * levels, width)
    level_index = jnp.arange(levels * NP2, dtype=jnp.int32) // NP2
    groups = elems // E_DEV

    def block_eval(inputs):
        owners, local_ids, coord_a, coord_b = inputs
        row_ids = ((owners * E_DEV + local_ids) * levels + level_index[None, :]).astype(jnp.int32)
        source = table[row_ids].reshape(row_ids.shape + (NP2, tracers))
        weights = lagrange_weights(coord_a, coord_b)
        interp = jnp.einsum("elk,elkq->elq", weights, source, precision=lax.Precision.HIGHEST)
        return interp, jnp.min(source, axis=2), jnp.max(source, axis=2)

    interp, lowest, highest = lax.map(block_eval, (dep_owner[..., 0].reshape(groups, E_DEV, -1), dep_local.reshape(groups, E_DEV, -1), dep_coord[0].reshape(groups, E_DEV, -1), dep_coord[1].reshape(groups, E_DEV, -1)))
    shape4 = (elems, levels, NP2, tracers)
    interp = interp.reshape(shape4)
    lowest = lowest.reshape(shape4)
    highest = highest.reshape(shape4)
    mass_new = new_mass.reshape(elems, levels, NP2, 1)
    source_total = jnp.sum(old_mass.reshape(elems, levels, NP2, 1) * tracer.reshape(shape4), axis=(0, 2))
    clipped, upper, lower, sums = fixer_terms(interp, lowest, highest, mass_new)
    result = apply_fix(clipped, upper, lower, source_total, sums[0], sums[1], sums[2])
    return result.reshape(elems, levels, width)
```

```python
import jax
import jax.numpy as jnp
from jax import lax
from jax.experimental import pallas as pl
from jax.experimental.pallas import tpu as pltpu
from jax.sharding import PartitionSpec as P

GLL = (-1.0, -0.4472135954999579, 0.4472135954999579, 1.0)
DEVS = 128
ELEMS = 8
LEVELS = 8
NODES = 16
Q = 40
SLOTS = 32
COLS = LEVELS * NODES
F32, BF16, I32 = jnp.float32, jnp.bfloat16, jnp.int32
NT = (((1,), (1,)), ((), ()))


def iota(shape, dim):
    return lax.broadcasted_iota(I32, shape, dim)


def dot(a, b):
    return jnp.dot(a, b, preferred_element_type=F32)


def dot_nt(a, b):
    return lax.dot_general(a, b, NT, preferred_element_type=F32)


def split2(x):
    high = x.astype(BF16)
    return high, (x - high.astype(F32)).astype(BF16)


def split3(x):
    high = x.astype(BF16)
    rest = x - high.astype(F32)
    mid = rest.astype(BF16)
    return high, mid, (rest - mid.astype(F32)).astype(BF16)


def pack_kernel(me_ref, owner_ref, local_ref, coord_ref, mass_ref, req_ref, idx_ref, peer_ref):
    me = me_ref[0]
    sub = iota((DEVS, COLS), 0)
    lane = iota((DEVS, COLS), 1)
    level = (iota((1, COLS), 1) // NODES).astype(F32)
    before = jnp.where(sub < lane, 1.0, 0.0).astype(BF16)
    counter = jnp.concatenate([before, jnp.ones((COLS, COLS), BF16)], axis=1)
    owners, hots = [], []
    for e in range(ELEMS):
        owner = owner_ref[e : e + 1, :]
        owner = jnp.where(owner == me, -1, owner)
        owners.append(owner)
        hots.append(jnp.where(jnp.broadcast_to(owner, (DEVS, COLS)) == sub, 1.0, 0.0))
    counts = dot(jnp.concatenate(hots, axis=0).astype(BF16), counter)
    total = counts[:DEVS, COLS:]
    for e in range(1, ELEMS):
        total = total + counts[e * DEVS : (e + 1) * DEVS, COLS:]
    present = jnp.where(total > 0.0, 1.0, 0.0)
    earlier = jnp.where(lane < sub, 1.0, 0.0).astype(BF16)
    peer = dot(earlier, present.astype(BF16))
    base = peer * 0.0
    slot = sub % SLOTS
    wide = []
    for e in range(ELEMS):
        part = counts[e * DEVS : (e + 1) * DEVS]
        place = (part[:, :COLS] + base) * 8.0 + peer
        base = base + part[:, COLS:]
        row = jnp.sum(hots[e] * place, axis=0, keepdims=True)
        idx_ref[e : e + 1, :] = jnp.where(owners[e] >= 0, row, -1.0)
        rank = row.astype(I32) // 8
        local = local_ref[e : e + 1, :].astype(F32) * float(LEVELS) + level
        values = (local, coord_ref[0, e : e + 1, :], coord_ref[1, e : e + 1, :], mass_ref[e : e + 1, :])
        value = jnp.concatenate([jnp.broadcast_to(v, (SLOTS, COLS)) for v in values], axis=0)
        wide.append(jnp.where(jnp.broadcast_to(rank, (DEVS, COLS)) == slot, value, 0.0))
    hot = jnp.concatenate(hots, axis=1).astype(BF16)
    high, mid, low = split3(jnp.concatenate(wide, axis=1))
    req_ref[...] = dot_nt(hot, high) + dot_nt(hot, mid) + dot_nt(hot, low)
    ids = []
    owner_id = sub.astype(F32)
    for p in range(8):
        mine = jnp.where(peer == float(p), present, 0.0)
        ids.append(jnp.sum(mine * owner_id, axis=0, keepdims=True))
    peer_ref[...] = jnp.concatenate(ids, axis=0).astype(I32)


def node_constants(n):
    def one(index):
        p0 = jnp.where(index > 0, GLL[0], GLL[1])
        p1 = jnp.where(index > 1, GLL[1], GLL[2])
        p2 = jnp.where(index > 2, GLL[2], GLL[3])
        scale = []
        for i in range(4):
            prod = 1.0
            for j in range(4):
                if j != i:
                    prod *= GLL[i] - GLL[j]
            scale.append(1.0 / prod)
        c = jnp.where(index == 0, scale[0], jnp.where(index == 1, scale[1], jnp.where(index == 2, scale[2], scale[3])))
        return p0, p1, p2, c

    k = iota((NODES, n), 0)
    return one(k // 4), one(k % 4)


def lagrange(x, consts):
    p0, p1, p2, c = consts
    return ((x - p0) * (x - p1)) * ((x - p2) * c)


def evaluate(row, a, b, mass, table, bounds, consts):
    n = row.shape[1]
    index = row.astype(I32)
    index8 = jnp.broadcast_to(index, (8, n))
    elem8 = index8 // LEVELS
    level8 = index8 % LEVELS
    w = lagrange(jnp.broadcast_to(a, (NODES, n)), consts[0]) * lagrange(jnp.broadcast_to(b, (NODES, n)), consts[1])
    wh = w.astype(BF16).astype(F32)
    wm = w - wh
    sh, sm = [], []
    for e in range(ELEMS):
        here = elem8 == e
        for h in range(2):
            sh.append(jnp.where(here, wh[8 * h : 8 * h + 8], 0.0))
            sm.append(jnp.where(here, wm[8 * h : 8 * h + 8], 0.0))
    sh = jnp.concatenate(sh, axis=0).astype(BF16)
    sm = jnp.concatenate(sm, axis=0).astype(BF16)
    r = dot(table, jnp.concatenate([sh, sm, sh], axis=0))
    hot = []
    sub8 = iota((8, n), 0)
    for e in range(ELEMS):
        hot.append(jnp.where(index8 == sub8 + 8 * e, 1.0, 0.0))
    hot = jnp.concatenate(hot, axis=0).astype(BF16)
    lim = dot(bounds, jnp.concatenate([hot, hot, hot], axis=0))
    at = [level8 == l for l in range(LEVELS)]
    clipped, highest, lowest = [], [], []
    for t in range(Q // 8):
        v = r[8 * t : 8 * t + 8]
        for l in range(1, LEVELS):
            v = jnp.where(at[l], r[l * Q + 8 * t : l * Q + 8 * t + 8], v)
        lo = lim[8 * t : 8 * t + 8]
        hi = lim[Q + 8 * t : Q + 8 * t + 8]
        clipped.append(jnp.minimum(jnp.maximum(v, lo), hi))
        highest.append(hi)
        lowest.append(lo)
    mass8 = jnp.broadcast_to(mass, (8, n))
    mh = mass8.astype(BF16).astype(F32)
    mm = mass8 - mh
    mine = level8 == sub8
    by_level = jnp.concatenate([jnp.where(mine, mh, 0.0), jnp.where(mine, mm, 0.0)], axis=0).astype(BF16)
    ch, cm = split2(jnp.concatenate(clipped, axis=0))
    sums = dot_nt(jnp.concatenate([ch, cm], axis=0), by_level)
    mmh = mm.astype(BF16).astype(F32)
    mass3 = jnp.where(sub8 == 0, mh, jnp.where(sub8 == 1, mmh, jnp.where(sub8 == 2, mm - mmh, 0.0)))
    hist = dot_nt(jnp.concatenate([mass3, mass3 * 0.0], axis=0).astype(BF16), hot)
    return clipped, highest, lowest, sums, hist


def spread_terms(clipped, highest, lowest):
    margin = 0.01 + 0.05 * (highest - lowest)
    return highest + margin - clipped, clipped - lowest + margin


def level_sums(sums, hist, low_table, high_table):
    s = sums[:Q] + sums[Q:]
    clip = s[:, :LEVELS] + s[:, LEVELS:]
    mass = hist[0:1] + hist[1:2] + hist[2:3]

    def fold(x):
        total = x[:, :LEVELS]
        for e in range(1, ELEMS):
            total = total + x[:, e * LEVELS : (e + 1) * LEVELS]
        return total

    s_low = fold(low_table * mass)
    s_high = fold(high_table * mass)
    margin = 0.01 * fold(jnp.broadcast_to(mass, (Q, mass.shape[1]))) + 0.05 * (s_high - s_low)
    return clip, s_high + margin - clip, clip - s_low + margin


def home_kernel(me_ref, t_ref, old_ref, owner_ref, local_ref, coord_ref, mass_ref, bt_ref, table_ref, bounds_ref, part_ref, c_ref, up_ref, down_ref):
    me = me_ref[0]
    t = t_ref[...]
    th, tm = split2(t)
    table = jnp.concatenate([th, th, tm], axis=1)
    table_ref[...] = table
    bh, bm, bl = split3(bt_ref[...])
    bounds = jnp.concatenate([bh, bm, bl], axis=1)
    bounds_ref[...] = bounds
    lane = iota((Q, COLS), 1)
    source = jnp.zeros((Q, COLS), F32)
    for l in range(LEVELS):
        s = jnp.sum(t[l * Q : (l + 1) * Q] * old_ref[l : l + 1, :], axis=1, keepdims=True)
        source = jnp.where(lane == l, s, source)
    level = iota((1, COLS), 1) // NODES
    n = 2 * COLS
    consts = node_constants(n)
    sums, hist = None, None
    for e in range(0, ELEMS, 2):

        def pair(f):
            return jnp.concatenate([f(e), f(e + 1)], axis=1)

        row = pair(lambda i: (local_ref[i : i + 1, :] * LEVELS + level).astype(F32))
        a = pair(lambda i: coord_ref[0, i : i + 1, :])
        b = pair(lambda i: coord_ref[1, i : i + 1, :])
        mass = pair(lambda i: jnp.where(owner_ref[i : i + 1, :] == me, mass_ref[i : i + 1, :], 0.0))
        clipped, highest, lowest, s, h = evaluate(row, a, b, mass, table, bounds, consts)
        sums = s if sums is None else sums + s
        hist = h if hist is None else hist + h
        for i in range(Q // 8):
            up, down = spread_terms(clipped[i], highest[i], lowest[i])
            for j in range(2):
                at = slice((e + j) * Q + 8 * i, (e + j) * Q + 8 * i + 8)
                c_ref[at, :] = clipped[i][:, j * COLS : (j + 1) * COLS]
                up_ref[at, :] = up[:, j * COLS : (j + 1) * COLS]
                down_ref[at, :] = down[:, j * COLS : (j + 1) * COLS]
    clip, up, down = level_sums(sums, hist, bt_ref[:Q, :], bt_ref[Q:, :])
    pad = jnp.zeros((Q, COLS - 3 * LEVELS), F32)
    part_ref[...] = jnp.concatenate([source[:, :LEVELS] - clip, up, down, pad], axis=1)


def serve_kernel(req_ref, table_ref, bounds_ref, part_ref, bt_ref, sums_ref, level_ref, c_ref, up_ref, down_ref):
    rows = req_ref[...].T
    level_ref[...] = (rows[:SLOTS].astype(I32) % LEVELS).astype(F32)
    table = table_ref[...]
    bounds = bounds_ref[...]
    consts = node_constants(2 * DEVS)
    sums, hist = None, None
    for s0 in range(0, SLOTS, 2):

        def pair(v):
            return jnp.concatenate([rows[v * SLOTS + s0 : v * SLOTS + s0 + 1], rows[v * SLOTS + s0 + 1 : v * SLOTS + s0 + 2]], axis=1)

        clipped, highest, lowest, s, h = evaluate(pair(0), pair(1), pair(2), pair(3), table, bounds, consts)
        sums = s if sums is None else sums + s
        hist = h if hist is None else hist + h
        for i in range(Q // 8):
            up, down = spread_terms(clipped[i], highest[i], lowest[i])
            for j in range(2):
                at = slice((s0 + j) * Q + 8 * i, (s0 + j) * Q + 8 * i + 8)
                c_ref[at, :] = clipped[i][:, j * DEVS : (j + 1) * DEVS]
                up_ref[at, :] = up[:, j * DEVS : (j + 1) * DEVS]
                down_ref[at, :] = down[:, j * DEVS : (j + 1) * DEVS]
    clip, up, down = level_sums(sums, hist, bt_ref[:Q, :], bt_ref[Q:, :])
    part = jnp.concatenate([-clip, up, down], axis=1) + part_ref[:, : 3 * LEVELS]
    packed = [part[8 * i : 8 * i + 8] for i in range(Q // 8)]
    packed.append(jnp.zeros((8, COLS - 3 * LEVELS * (Q // 8)), F32))
    packed = jnp.concatenate(packed, axis=1)
    for d in range(DEVS):
        sums_ref[8 * d : 8 * d + 8, :] = packed


def finish_kernel(tot_ref, level_ref, c_ref, up_ref, down_ref, ans_ref, home_ref, out_scratch):
    total = tot_ref[0:8, :]
    for d in range(1, DEVS):
        total = total + tot_ref[8 * d : 8 * d + 8, :]
    up_total = pltpu.roll(total, COLS - LEVELS, 1)
    down_total = pltpu.roll(total, COLS - 2 * LEVELS, 1)
    rise = jnp.maximum(total, 0.0) / up_total
    fall = jnp.minimum(total, 0.0) / down_total
    home_level = iota((8, COLS), 1) // NODES
    for i in range(Q // 8):
        rises = [jnp.broadcast_to(rise[:, 24 * i + l : 24 * i + l + 1], (8, DEVS)) for l in range(LEVELS)]
        falls = [jnp.broadcast_to(fall[:, 24 * i + l : 24 * i + l + 1], (8, DEVS)) for l in range(LEVELS)]
        hr, hf = rises[0], falls[0]
        for l in range(1, LEVELS):
            hr = jnp.where(home_level == l, rises[l], hr)
            hf = jnp.where(home_level == l, falls[l], hf)
        home_ref[8 * i : 8 * i + 8, :] = hr
        home_ref[Q + 8 * i : Q + 8 * i + 8, :] = hf
        for s in range(SLOTS):
            level8 = jnp.broadcast_to(level_ref[s : s + 1, :].astype(I32), (8, DEVS))
            r, f = rises[0], falls[0]
            for l in range(1, LEVELS):
                r = jnp.where(level8 == l, rises[l], r)
                f = jnp.where(level8 == l, falls[l], f)
            at = slice(s * Q + 8 * i, s * Q + 8 * i + 8)
            out_scratch[at, :] = c_ref[at, :] + r * up_ref[at, :] + f * down_ref[at, :]
    for j in range(SLOTS * Q // 128):
        ans_ref[pl.ds(j, DEVS, stride=SLOTS * Q // 128), :] = out_scratch[128 * j : 128 * (j + 1), :].T


def place_kernel(idx_ref, hot_ref, scratch):
    cols = jnp.concatenate([idx_ref[...], jnp.full((COLS - ELEMS, COLS), -1.0, F32)], axis=0).T
    scratch[...] = cols
    turned = jnp.concatenate([scratch[pl.ds(k, LEVELS, stride=NODES), :] for k in range(NODES)], axis=0)
    lane = iota((COLS, SLOTS * 8), 1).astype(F32)
    for e in range(ELEMS):
        col = jnp.broadcast_to(turned[:, e : e + 1], (COLS, SLOTS * 8))
        hot_ref[e * COLS : (e + 1) * COLS, :] = jnp.where(col == lane, 1.0, 0.0).astype(BF16)


def home_finish_kernel(coef_ref, idx_ref, c_ref, up_ref, down_ref, out_ref, scratch):
    for e in range(ELEMS):
        at = slice(e * Q, (e + 1) * Q)
        v = c_ref[at, :] + coef_ref[:Q, :] * up_ref[at, :] + coef_ref[Q:, :] * down_ref[at, :]
        v = jnp.where(jnp.broadcast_to(idx_ref[e : e + 1, :], (Q, COLS)) < 0.0, v, 0.0)
        scratch[e] = jnp.concatenate([v, jnp.zeros((COLS - Q, COLS), F32)], axis=0).T
        for k in range(NODES):
            out_ref[e * COLS + 8 * k : e * COLS + 8 * k + 8, :] = scratch[e, pl.ds(k, LEVELS, stride=NODES), :]


def join_kernel(peer_ref, ans_ref, hot_ref, home_ref, out_ref, rows, sem):
    chunk = SLOTS * Q // 128
    copies = [
        pltpu.make_async_copy(ans_ref.at[pl.ds(peer_ref[p, 0] * chunk, chunk), :], rows.at[pl.ds(p * chunk, chunk), :], sem.at[p])
        for p in range(5)
    ]
    for copy in copies:
        copy.start()
    rows[5 * chunk :, :] = jnp.zeros((3 * chunk, 128), F32)
    for copy in copies:
        copy.wait()
    flat = jnp.concatenate([rows[pl.ds(j, 8, stride=chunk), :] for j in range(chunk)], axis=1)
    table = jnp.concatenate([flat[:, s * Q : (s + 1) * Q] for s in range(SLOTS)], axis=0)
    high, mid = split2(table)
    for e in range(ELEMS):
        hot = hot_ref[e * COLS : (e + 1) * COLS, :]
        v = dot(hot, high) + dot(hot, mid) + home_ref[e * COLS : (e + 1) * COLS, :Q]
        out_ref[e] = jnp.concatenate([v[8 * k : 8 * k + 8] for k in range(NODES)], axis=1)


def body(tracer, old_mass, new_mass, dep_owner, dep_local, dep_coord):
    me = lax.axis_index("elem").astype(I32).reshape(1)
    owner = dep_owner.reshape(ELEMS, COLS)
    vmem = pl.BlockSpec(memory_space=pltpu.VMEM)
    smem = pl.BlockSpec(memory_space=pltpu.SMEM)

    def shape(rows, cols, dtype=F32):
        return jax.ShapeDtypeStruct((rows, cols), dtype)

    def exchange(x, chunk):
        y = lax.all_to_all(x.reshape((DEVS,) + chunk), "elem", 0, 0, tiled=True)
        return y.reshape(x.shape)

    req, idx, peer = pl.pallas_call(
        pack_kernel,
        out_shape=(shape(DEVS, COLS), shape(ELEMS, COLS), shape(8, COLS, I32)),
        in_specs=[smem] + [vmem] * 4,
        out_specs=(vmem,) * 3,
        name="pack",
    )(me, owner, dep_local, dep_coord, new_mass)
    asked = exchange(req, (1, COLS))

    nodes = tracer.reshape(ELEMS, LEVELS, NODES, Q)
    t = jnp.transpose(nodes, (1, 3, 0, 2)).reshape(LEVELS * Q, ELEMS * NODES)
    old = jnp.transpose(old_mass.reshape(ELEMS, LEVELS, NODES), (1, 0, 2)).reshape(LEVELS, COLS)
    bt = jnp.concatenate([jnp.min(nodes, axis=2), jnp.max(nodes, axis=2)], axis=-1).reshape(ELEMS * LEVELS, 2 * Q).T
    table, bounds, part, hc, hu, hd = pl.pallas_call(
        home_kernel,
        out_shape=(shape(LEVELS * Q, 3 * COLS, BF16), shape(2 * Q, 3 * ELEMS * LEVELS, BF16), shape(Q, COLS))
        + (shape(ELEMS * Q, COLS),) * 3,
        in_specs=[smem] + [vmem] * 7,
        out_specs=(vmem,) * 6,
        name="home",
    )(me, t, old, owner, dep_local, dep_coord, new_mass, bt)

    sums, level, c, up, down = pl.pallas_call(
        serve_kernel,
        out_shape=(shape(8 * DEVS, COLS), shape(SLOTS, DEVS)) + (shape(SLOTS * Q, DEVS),) * 3,
        in_specs=[vmem] * 5,
        out_specs=(vmem,) * 5,
        name="serve",
    )(asked, table, bounds, part, bt)
    totals = exchange(sums, (8, COLS))

    hot = pl.pallas_call(
        place_kernel,
        out_shape=shape(ELEMS * COLS, SLOTS * 8, BF16),
        in_specs=[vmem],
        out_specs=vmem,
        scratch_shapes=[pltpu.VMEM((COLS, COLS), F32)],
        name="place",
    )(idx)

    ans, coef = pl.pallas_call(
        finish_kernel,
        out_shape=(shape(SLOTS * Q * DEVS // 128, 128), shape(2 * Q, COLS)),
        in_specs=[vmem] * 5,
        out_specs=(vmem,) * 2,
        scratch_shapes=[pltpu.VMEM((SLOTS * Q, DEVS), F32)],
        name="finish",
    )(totals, level, c, up, down)
    got = exchange(ans, (1, SLOTS * Q))

    home = pl.pallas_call(
        home_finish_kernel,
        out_shape=shape(ELEMS * COLS, 128),
        in_specs=[vmem] * 5,
        out_specs=vmem,
        scratch_shapes=[pltpu.VMEM((ELEMS, COLS, 128), F32)],
        name="home_finish",
    )(coef, idx, hc, hu, hd)

    return pl.pallas_call(
        join_kernel,
        out_shape=jax.ShapeDtypeStruct((ELEMS, LEVELS, NODES * Q), F32),
        in_specs=[smem, pl.BlockSpec(memory_space=pl.ANY), vmem, vmem],
        out_specs=vmem,
        scratch_shapes=[pltpu.VMEM((8 * SLOTS * Q // 128, 128), F32), pltpu.SemaphoreType.DMA((5,))],
        name="join",
    )(peer, got, hot, home)


def solution(mesh):
    placed = (
        P("elem", None, None),
        P("elem", None),
        P("elem", None),
        P("elem", None, None),
        P("elem", None),
        P(None, "elem", None),
    )
    return jax.shard_map(body, mesh=mesh, in_specs=placed, out_specs=P("elem", None, None), check_vma=False)
```

```python
import jax
import jax.numpy as jnp
from jax import lax
from jax.experimental import pallas as pl
from jax.experimental.pallas import tpu as pltpu
from jax.sharding import PartitionSpec as P

GLL = (-1.0, -0.4472135954999579, 0.4472135954999579, 1.0)
DEVS = 128
ELEMS = 8
LEVELS = 8
NODES = 16
Q = 40
SLOTS = 32
PEERS = 5
COLS = LEVELS * NODES
CHUNK = SLOTS * Q // 128
F32, BF16, I32 = jnp.float32, jnp.bfloat16, jnp.int32
NT = (((1,), (1,)), ((), ()))


def iota(shape, dim):
    return lax.broadcasted_iota(I32, shape, dim)


def dot(a, b):
    return jnp.dot(a, b, preferred_element_type=F32)


def dot_nt(a, b):
    return lax.dot_general(a, b, NT, preferred_element_type=F32)


def split2(x):
    high = x.astype(BF16)
    return high, (x - high.astype(F32)).astype(BF16)


def split3(x):
    high = x.astype(BF16)
    rest = x - high.astype(F32)
    mid = rest.astype(BF16)
    return high, mid, (rest - mid.astype(F32)).astype(BF16)


def pack_kernel(me_ref, owner_hbm, local_hbm, coord_hbm, mass_hbm, old_hbm, tracer_hbm, req_ref, idx_ref, peer_ref, vals_ref, old_ref, tracer_ref, owner_ref, local_ref, coord_ref, mass_ref, sem):
    pairs = (
        (owner_hbm, owner_ref),
        (local_hbm, local_ref),
        (coord_hbm, coord_ref),
        (mass_hbm, mass_ref),
        (old_hbm, old_ref),
        (tracer_hbm, tracer_ref),
    )
    copies = [pltpu.make_async_copy(src, dst, sem.at[i]) for i, (src, dst) in enumerate(pairs)]
    for copy in copies:
        copy.start()
    me = me_ref[0]
    sub = iota((DEVS, COLS), 0)
    lane = iota((DEVS, COLS), 1)
    before = jnp.where(sub < lane, 1.0, 0.0).astype(BF16)
    counter = jnp.concatenate([before, jnp.ones((COLS, COLS), BF16)], axis=1)
    earlier = jnp.where(lane < sub, 1.0, 0.0).astype(BF16)
    for copy in copies[:4]:
        copy.wait()
    owner = owner_ref[...]
    away = owner != me
    owner = jnp.where(away, owner, -1)
    level = iota((ELEMS, COLS), 1) // NODES
    row = (local_ref[...] * LEVELS + (level + 1)).astype(F32)
    mass = mass_ref[...]
    vals_ref[:ELEMS] = row
    vals_ref[ELEMS : 2 * ELEMS] = coord_ref[0]
    vals_ref[2 * ELEMS : 3 * ELEMS] = coord_ref[1]
    vals_ref[3 * ELEMS :] = jnp.where(away, 0.0, mass)
    values = (row, coord_ref[0], coord_ref[1], mass)
    hots = [jnp.where(jnp.broadcast_to(owner[e : e + 1], (DEVS, COLS)) == sub, 1.0, 0.0) for e in range(ELEMS)]
    counts = dot(jnp.concatenate(hots, axis=0).astype(BF16), counter)
    total = counts[:DEVS, COLS:]
    for e in range(1, ELEMS):
        total = total + counts[e * DEVS : (e + 1) * DEVS, COLS:]
    present = jnp.where(total > 0.0, 1.0, 0.0)
    peer = dot(earlier, present.astype(BF16))
    base = peer * float(SLOTS)
    slot = sub % SLOTS
    wide, places = [], []
    for e in range(ELEMS):
        part = counts[e * DEVS : (e + 1) * DEVS]
        place = part[:, :COLS] + base
        base = base + part[:, COLS:]
        spot = jnp.sum(hots[e] * place, axis=0, keepdims=True).astype(I32)
        places.append(spot)
        value = jnp.concatenate([jnp.broadcast_to(v[e : e + 1], (SLOTS, COLS)) for v in values], axis=0)
        wide.append(jnp.where(jnp.broadcast_to(spot % SLOTS, (DEVS, COLS)) == slot, value, 0.0))
    idx_ref[...] = jnp.where(away, jnp.concatenate(places, axis=0), -1).astype(F32)
    hot = jnp.concatenate(hots, axis=1).astype(BF16)
    high, mid = split2(jnp.concatenate(wide, axis=1))
    req_ref[...] = dot_nt(hot, high) + dot_nt(hot, mid)
    owner_id = sub.astype(F32)
    ids = [jnp.sum(jnp.where(peer == float(p), present, 0.0) * owner_id, axis=0, keepdims=True) for p in range(PEERS)]
    named = jnp.sum(present, axis=0, keepdims=True)
    ids = [ids[0]] + [jnp.where(named > float(p), ids[p], ids[0]) for p in range(1, PEERS)]
    peer_ref[...] = jnp.concatenate(ids + [named] * (8 - PEERS), axis=0).astype(I32)
    for copy in copies[4:]:
        copy.wait()


def node_constants(n):
    def one(index):
        p0 = jnp.where(index > 0, GLL[0], GLL[1])
        p1 = jnp.where(index > 1, GLL[1], GLL[2])
        p2 = jnp.where(index > 2, GLL[2], GLL[3])
        scale = []
        for i in range(4):
            prod = 1.0
            for j in range(4):
                if j != i:
                    prod *= GLL[i] - GLL[j]
            scale.append(1.0 / prod)
        c = jnp.where(index == 0, scale[0], jnp.where(index == 1, scale[1], jnp.where(index == 2, scale[2], scale[3])))
        return p0, p1, p2, c

    k = iota((NODES, n), 0)
    return one(k // 4), one(k % 4)


def lagrange(x, consts):
    p0, p1, p2, c = consts
    return ((x - p0) * (x - p1)) * ((x - p2) * c)


def evaluate(row, a, b, mass, table, consts):
    n = row.shape[1]
    index = jnp.maximum(row.astype(I32) - 1, 0)
    index8 = jnp.broadcast_to(index, (8, n))
    level8 = index8 % LEVELS
    sub8 = iota((8, n), 0)
    hot = jnp.concatenate([jnp.where(index8 == sub8 + 8 * e, 1.0, 0.0) for e in range(ELEMS)], axis=0).astype(BF16)
    values = dot(table, jnp.concatenate([hot, hot, hot], axis=0))
    w = lagrange(jnp.broadcast_to(a, (NODES, n)), consts[0]) * lagrange(jnp.broadcast_to(b, (NODES, n)), consts[1])
    weights = [jnp.broadcast_to(w[k : k + 1], (8, n)) for k in range(NODES)]
    clipped, highest, lowest = [], [], []
    for t in range(Q // 8):
        v = values[8 * t : 8 * t + 8]
        total, low, high = weights[0] * v, v, v
        for k in range(1, NODES):
            v = values[k * Q + 8 * t : k * Q + 8 * t + 8]
            total = total + weights[k] * v
            low = jnp.minimum(low, v)
            high = jnp.maximum(high, v)
        clipped.append(jnp.minimum(jnp.maximum(total, low), high))
        highest.append(high)
        lowest.append(low)
    mass8 = jnp.broadcast_to(mass, (8, n))
    mh = mass8.astype(BF16).astype(F32)
    mm = mass8 - mh
    mine = level8 == sub8
    by_level = jnp.concatenate([jnp.where(mine, mh, 0.0), jnp.where(mine, mm, 0.0)], axis=0).astype(BF16)
    ch, cm = split2(jnp.concatenate(clipped, axis=0))
    sums = dot_nt(jnp.concatenate([ch, cm], axis=0), by_level)
    mmh = mm.astype(BF16).astype(F32)
    mass3 = jnp.where(sub8 == 0, mh, jnp.where(sub8 == 1, mmh, jnp.where(sub8 == 2, mm - mmh, 0.0)))
    hist = dot_nt(jnp.concatenate([mass3, mass3 * 0.0], axis=0).astype(BF16), hot)
    return clipped, highest, lowest, sums, hist, level8


def spread_terms(clipped, highest, lowest):
    margin = 0.01 + 0.05 * (highest - lowest)
    return highest + margin - clipped, clipped - lowest + margin


def fold(x):
    total = x[:, :LEVELS]
    for e in range(1, ELEMS):
        total = total + x[:, e * LEVELS : (e + 1) * LEVELS]
    return total


def level_sums(sums, hist, low_table, high_table):
    s = sums[:Q] + sums[Q:]
    clip = s[:, :LEVELS] + s[:, LEVELS:]
    mass = hist[0:1] + hist[1:2] + hist[2:3]

    s_low = fold(low_table * mass)
    s_high = fold(high_table * mass)
    margin = 0.01 * fold(jnp.broadcast_to(mass, (Q, mass.shape[1]))) + 0.05 * (s_high - s_low)
    return clip, s_high + margin - clip, clip - s_low + margin


def home_kernel(tracer_ref, old_ref, vals_ref, idx_ref, table_ref, bt_ref, part_ref, hot_ref, c_ref, up_ref, down_ref, scratch):
    rows = ELEMS * LEVELS
    node = iota((NODES, COLS), 0)
    column = iota((NODES, COLS), 1)
    wide = jnp.concatenate([jnp.where(column % NODES == node, jnp.broadcast_to(old_ref[e : e + 1, :], (NODES, COLS)), 0.0) for e in range(ELEMS)], axis=1)
    source_of = iota((ELEMS * COLS, rows), 0)
    gather = jnp.where(source_of // NODES == iota((ELEMS * COLS, rows), 1), 1.0, 0.0).astype(BF16)
    old = sum(dot(part, gather) for part in split3(wide))
    natural = tracer_ref[...].reshape(rows, NODES * Q)
    flat = [natural[:, 128 * j : 128 * (j + 1)].T for j in range(NODES * Q // 128)]
    for j, piece in enumerate(flat):
        table_ref[128 * j : 128 * (j + 1), :] = jnp.concatenate(split3(piece), axis=1)
    flat = jnp.concatenate(flat, axis=0)
    source = low = high = None
    for k in range(NODES):
        v = flat[k * Q : (k + 1) * Q]
        term = v * old[k : k + 1, :]
        source = term if source is None else source + term
        low = v if low is None else jnp.minimum(low, v)
        high = v if high is None else jnp.maximum(high, v)
    bt_ref[:Q] = low
    bt_ref[Q:] = high
    consts = node_constants(2 * COLS)
    table = table_ref[...]
    sums, hist = None, None
    for e in range(0, ELEMS, 2):
        args = [jnp.concatenate([vals_ref[v * ELEMS + e : v * ELEMS + e + 1], vals_ref[v * ELEMS + e + 1 : v * ELEMS + e + 2]], axis=1) for v in range(4)]
        clipped, highest, lowest, s, h, _ = evaluate(*args, table, consts)
        sums = s if sums is None else sums + s
        hist = h if hist is None else hist + h
        for i in range(Q // 8):
            up, down = spread_terms(clipped[i], highest[i], lowest[i])
            for j in range(2):
                at = slice((e + j) * Q + 8 * i, (e + j) * Q + 8 * i + 8)
                c_ref[at, :] = clipped[i][:, j * COLS : (j + 1) * COLS]
                up_ref[at, :] = up[:, j * COLS : (j + 1) * COLS]
                down_ref[at, :] = down[:, j * COLS : (j + 1) * COLS]
    clip, up, down = level_sums(sums, hist, low, high)
    pad = jnp.zeros((Q, COLS - 3 * LEVELS), F32)
    part_ref[...] = jnp.concatenate([fold(source) - clip, up, down, pad], axis=1)
    scratch[...] = jnp.concatenate([idx_ref[...], jnp.full((COLS - ELEMS, COLS), -1.0, F32)], axis=0).T
    turned = jnp.concatenate([scratch[pl.ds(k, LEVELS, stride=NODES), :] for k in range(NODES)], axis=0)
    lane = iota((COLS, SLOTS * 8), 1).astype(F32)
    for e in range(ELEMS):
        col = jnp.broadcast_to(turned[:, e : e + 1], (COLS, SLOTS * 8))
        hot_ref[e * COLS : (e + 1) * COLS, :] = jnp.where(col == lane, 1.0, 0.0).astype(BF16)


def serve_kernel(me_ref, req_ref, table_ref, part_ref, bt_ref, sums_ref, ids_ref, level_ref, c_ref, up_ref, down_ref, dense, tiles):
    req = req_ref[...]
    sub = iota((DEVS, DEVS), 0)
    lane = iota((DEVS, DEVS), 1)
    high, mid = split2(req)
    first = jnp.where(iota((16, DEVS), 1) == 0, 1.0, 0.0).astype(BF16)
    asks = jnp.where(dot_nt(first, high) > 0.0, 1.0, 0.0)
    place = dot(asks.astype(BF16), jnp.where(sub < lane, 1.0, 0.0).astype(BF16))
    count = jnp.sum(asks[0:1]).astype(I32)
    pick = jnp.where(jnp.broadcast_to(place[0:1], (DEVS, DEVS)) == sub.astype(F32), jnp.broadcast_to(asks[0:1], (DEVS, DEVS)), 0.0).astype(BF16)
    dense[...] = dot(pick, high) + dot(pick, mid)
    ids = dot_nt(iota((16, DEVS), 1).astype(F32).astype(BF16), pick)[:8].astype(I32)
    ids = jnp.where(iota((8, DEVS), 1) < count, ids, me_ref[0])
    ids_ref[...] = jnp.where(iota((8, DEVS), 0) == 0, ids, count)
    groups = [dense[pl.ds(i, DEVS // 4, stride=4), :] for i in range(4)]
    block = iota((DEVS // 4, DEVS), 1) // SLOTS
    for v in range(4):
        tile = None
        for i in range(4):
            shift = (i - v) * SLOTS % DEVS
            moved = pltpu.roll(groups[i], shift, 1) if shift else groups[i]
            tile = moved if tile is None else jnp.where(block == i, moved, tile)
        tiles[v] = tile
    consts = node_constants(2 * DEVS)

    def step(u, carry):
        args = [jnp.concatenate([tiles[v, pl.ds(2 * u, 1), :], tiles[v, pl.ds(2 * u + 1, 1), :]], axis=1) for v in range(4)]
        clipped, highest, lowest, s, h, level8 = evaluate(*args, table_ref[...], consts)
        for j in range(2):
            level_ref[pl.ds(pl.multiple_of(16 * u + 8 * j, 8), 8), :] = level8[:, j * DEVS : (j + 1) * DEVS]
        for i in range(Q // 8):
            up, down = spread_terms(clipped[i], highest[i], lowest[i])
            for j in range(2):
                at = pl.ds(pl.multiple_of(2 * Q * u + j * Q + 8 * i, 8), 8)
                c_ref[at, :] = clipped[i][:, j * DEVS : (j + 1) * DEVS]
                up_ref[at, :] = up[:, j * DEVS : (j + 1) * DEVS]
                down_ref[at, :] = down[:, j * DEVS : (j + 1) * DEVS]
        return carry[0] + s, carry[1] + h

    start = (jnp.zeros((2 * Q, 2 * LEVELS), F32), jnp.zeros((16, ELEMS * LEVELS), F32))
    sums, hist = lax.fori_loop(0, (count + 7) // 8, step, start)
    clip, up, down = level_sums(sums, hist, bt_ref[:Q, :], bt_ref[Q:, :])
    part = jnp.concatenate([-clip, up, down], axis=1) + part_ref[:, : 3 * LEVELS]
    packed = [part[8 * i : 8 * i + 8] for i in range(Q // 8)]
    packed.append(jnp.zeros((8, COLS - 3 * LEVELS * (Q // 8)), F32))
    packed = jnp.concatenate(packed, axis=1)
    for d in range(DEVS):
        sums_ref[8 * d : 8 * d + 8, :] = packed


def finish_kernel(ids_ref, tot_ref, level_ref, c_ref, up_ref, down_ref, idx_ref, hc_ref, hu_ref, hd_ref, ans_ref, home_ref, rises, falls, scratch):
    total = tot_ref[0:8, :]
    for d in range(1, DEVS):
        total = total + tot_ref[8 * d : 8 * d + 8, :]
    up_total = pltpu.roll(total, COLS - LEVELS, 1)
    down_total = pltpu.roll(total, COLS - 2 * LEVELS, 1)
    rise = jnp.maximum(total, 0.0) / up_total
    fall = jnp.minimum(total, 0.0) / down_total
    home_level = iota((8, COLS), 1) // NODES
    home_rise, home_fall = [], []
    for i in range(Q // 8):
        hr = hf = None
        for l in range(LEVELS):
            r = jnp.broadcast_to(rise[:, 24 * i + l : 24 * i + l + 1], (8, DEVS))
            f = jnp.broadcast_to(fall[:, 24 * i + l : 24 * i + l + 1], (8, DEVS))
            rises[i, l] = r
            falls[i, l] = f
            hr = r if hr is None else jnp.where(home_level == l, r, hr)
            hf = f if hf is None else jnp.where(home_level == l, f, hf)
        home_rise.append(hr)
        home_fall.append(hf)
    home_rise = jnp.concatenate(home_rise, axis=0)
    home_fall = jnp.concatenate(home_fall, axis=0)
    block = iota((CHUNK, DEVS), 1) // SLOTS

    def step(t, carry):
        level8 = level_ref[pl.ds(pl.multiple_of(8 * t, 8), 8), :]
        at_level = [level8 == l for l in range(LEVELS)]
        out = []
        for i in range(Q // 8):
            r, f = rises[i, 0], falls[i, 0]
            for l in range(1, LEVELS):
                r = jnp.where(at_level[l], rises[i, l], r)
                f = jnp.where(at_level[l], falls[i, l], f)
            at = pl.ds(pl.multiple_of(Q * t + 8 * i, 8), 8)
            out.append(c_ref[at, :] + r * up_ref[at, :] + f * down_ref[at, :])
        out = jnp.concatenate(out, axis=0)
        parts = [out[CHUNK * b : CHUNK * (b + 1)] for b in range(4)]
        for i in range(4):
            chunk = None
            for b in range(4):
                shift = (b - i) * SLOTS % DEVS
                moved = pltpu.roll(parts[b], shift, 1) if shift else parts[b]
                chunk = moved if chunk is None else jnp.where(block == b, moved, chunk)
            ans_ref[pl.ds(ids_ref[0, 4 * t + i] * CHUNK, CHUNK), :] = chunk
        return carry

    lax.fori_loop(0, (ids_ref[1, 0] + 3) // 4, step, 0)
    for e in range(ELEMS):
        at = slice(e * Q, (e + 1) * Q)
        v = hc_ref[at, :] + home_rise * hu_ref[at, :] + home_fall * hd_ref[at, :]
        v = jnp.where(jnp.broadcast_to(idx_ref[e : e + 1, :], (Q, COLS)) < 0.0, v, 0.0)
        scratch[e] = jnp.concatenate([v, jnp.zeros((COLS - Q, COLS), F32)], axis=0).T
        for k in range(NODES):
            home_ref[e * COLS + 8 * k : e * COLS + 8 * k + 8, :] = scratch[e, pl.ds(k, LEVELS, stride=NODES), :]


def join_kernel(peer_ref, ans_ref, hot_ref, home_ref, out_hbm, out_ref, sem):
    block = iota((CHUNK, 128), 1) // SLOTS
    chunks = [ans_ref[pl.ds(peer_ref[p, 0] * CHUNK, CHUNK), :] for p in range(PEERS)]
    table = []
    for b in range(4):

        def moved(p):
            shift = (p - b) * SLOTS % 128
            return pltpu.roll(chunks[p], shift, 1) if shift else chunks[p]

        near = moved(0)
        for p in range(1, 4):
            near = jnp.where(block == p, moved(p), near)
        table.append(jnp.concatenate([near, jnp.where(block == 0, moved(4), 0.0)], axis=1))
    high, mid = split2(jnp.concatenate(table, axis=0))
    for e in range(ELEMS):
        hot = hot_ref[e * COLS : (e + 1) * COLS, :]
        v = dot_nt(hot, high) + dot_nt(hot, mid) + home_ref[e * COLS : (e + 1) * COLS, :Q]
        out_ref[e] = jnp.concatenate([v[8 * k : 8 * k + 8] for k in range(NODES)], axis=1)
        pltpu.make_async_copy(out_ref.at[e], out_hbm.at[e], sem.at[e]).start()
    for e in range(ELEMS):
        pltpu.make_async_copy(out_ref.at[e], out_hbm.at[e], sem.at[e]).wait()


def body(tracer, old_mass, new_mass, dep_owner, dep_local, dep_coord):
    me = lax.axis_index("elem").astype(I32).reshape(1)
    owner = dep_owner.reshape(ELEMS, COLS)
    smem, vmem, hbm = (pl.BlockSpec(memory_space=m) for m in (pltpu.SMEM, pltpu.VMEM, pltpu.HBM))

    def near(*arrays):
        return [pltpu.with_memory_space_constraint(x, pltpu.VMEM) for x in arrays]

    def call(kernel, name, outs, in_specs, scratch, args):
        return pl.pallas_call(
            kernel,
            out_shape=tuple(pltpu.VMEM(shape, dtype) for shape, dtype in outs),
            in_specs=in_specs,
            out_specs=(vmem,) * len(outs),
            scratch_shapes=scratch,
            compiler_params=pltpu.CompilerParams(vmem_limit_bytes=20 << 20),
            name=name,
        )(*args)

    def exchange(x, chunk):
        y = lax.all_to_all(x.reshape((DEVS,) + chunk), "elem", 0, 0, tiled=True)
        return y.reshape(x.shape)

    req, idx, peer, vals, old, table_in = call(
        pack_kernel,
        "pack",
        (
            ((DEVS, COLS), F32),
            ((ELEMS, COLS), F32),
            ((8, COLS), I32),
            ((4 * ELEMS, COLS), F32),
            ((ELEMS, COLS), F32),
            (tracer.shape, F32),
        ),
        [smem] + [hbm] * 6,
        [
            pltpu.VMEM((ELEMS, COLS), I32),
            pltpu.VMEM((ELEMS, COLS), I32),
            pltpu.VMEM((2, ELEMS, COLS), F32),
            pltpu.VMEM((ELEMS, COLS), F32),
            pltpu.SemaphoreType.DMA((6,)),
        ],
        [me] + [pltpu.with_memory_space_constraint(x, pltpu.HBM) for x in (owner, dep_local, dep_coord, new_mass, old_mass, tracer)],
    )
    asked = exchange(req, (1, COLS))
    table, bt, part, hot, hc, hu, hd = call(
        home_kernel,
        "home",
        (
            ((NODES * Q, 3 * ELEMS * LEVELS), BF16),
            ((2 * Q, ELEMS * LEVELS), F32),
            ((Q, COLS), F32),
            ((ELEMS * COLS, SLOTS * 8), BF16),
        )
        + (((ELEMS * Q, COLS), F32),) * 3,
        [vmem] * 4,
        [pltpu.VMEM((COLS, COLS), F32)],
        near(table_in, old, vals, idx),
    )
    sums, ids, level, c, up, down = call(
        serve_kernel,
        "serve",
        (((8 * DEVS, COLS), F32), ((8, DEVS), I32), ((2 * DEVS, DEVS), I32)) + (((SLOTS * Q, DEVS), F32),) * 3,
        [smem] + [vmem] * 4,
        [pltpu.VMEM((DEVS, DEVS), F32), pltpu.VMEM((4, DEVS // 4, DEVS), F32)],
        [me] + near(asked, table, part, bt),
    )
    totals = exchange(sums, (8, COLS))
    ans, home = call(
        finish_kernel,
        "finish",
        (((DEVS * CHUNK, 128), F32), ((ELEMS * COLS, 128), F32)),
        [smem] + [vmem] * 9,
        [pltpu.VMEM((Q // 8, LEVELS, 8, DEVS), F32)] * 2 + [pltpu.VMEM((ELEMS, COLS, 128), F32)],
        [ids] + near(totals, level, c, up, down, idx, hc, hu, hd),
    )
    got = exchange(ans, (1, SLOTS * Q))
    return pl.pallas_call(
        join_kernel,
        out_shape=jax.ShapeDtypeStruct((ELEMS, LEVELS, NODES * Q), F32),
        in_specs=[smem] + [vmem] * 3,
        out_specs=hbm,
        scratch_shapes=[pltpu.VMEM((ELEMS, LEVELS, NODES * Q), F32), pltpu.SemaphoreType.DMA((ELEMS,))],
        compiler_params=pltpu.CompilerParams(vmem_limit_bytes=20 << 20),
        name="join",
    )(peer, *near(got, hot, home))


def solution(mesh):
    placed = (
        P("elem", None, None),
        P("elem", None),
        P("elem", None),
        P("elem", None, None),
        P("elem", None),
        P(None, "elem", None),
    )
    return jax.shard_map(body, mesh=mesh, in_specs=placed, out_specs=P("elem", None, None), check_vma=False)
```

```python
import jax
import jax.numpy as jnp
from jax import lax
from jax.experimental import pallas as pl
from jax.experimental.pallas import tpu as pltpu
from jax.sharding import Mesh
from jax.sharding import PartitionSpec as P

AXES = ("x", "y", "z", "core")
GROUP = ("core", "z", "y", "x")
GLL = (-1.0, -0.4472135954999579, 0.4472135954999579, 1.0)
DEVS = 128
ELEMS = 8
LEVELS = 8
NODES = 16
Q = 40
SLOTS = 32
PEERS = 5
COLS = LEVELS * NODES
CHUNK = SLOTS * Q // 128
F32, BF16, I32 = jnp.float32, jnp.bfloat16, jnp.int32
NT = (((1,), (1,)), ((), ()))


def iota(shape, dim):
    return lax.broadcasted_iota(I32, shape, dim)


def in_group(device):
    core, z, y, x = device % 2, device // 2 % 4, device // 8 % 4, device // 32
    return core * 64 + z * 16 + y * 4 + x


def dot(a, b):
    return jnp.dot(a, b, preferred_element_type=F32)


def dot_nt(a, b):
    return lax.dot_general(a, b, NT, preferred_element_type=F32)


def split2(x):
    high = x.astype(BF16)
    return high, (x - high.astype(F32)).astype(BF16)


def split3(x):
    high = x.astype(BF16)
    rest = x - high.astype(F32)
    mid = rest.astype(BF16)
    return high, mid, (rest - mid.astype(F32)).astype(BF16)


def ranks(owner):
    sub = iota((DEVS, COLS), 0)
    before = jnp.where(sub < iota((DEVS, COLS), 1), 1.0, 0.0).astype(BF16)
    counter = jnp.concatenate([before, jnp.ones((COLS, COLS), BF16)], axis=1)
    hots = [jnp.where(jnp.broadcast_to(owner[e : e + 1], (DEVS, COLS)) == sub, 1.0, 0.0) for e in range(ELEMS)]
    counts = dot(jnp.concatenate(hots, axis=0).astype(BF16), counter)
    parts = [counts[e * DEVS : (e + 1) * DEVS] for e in range(ELEMS)]
    return hots, [p[:, :COLS] for p in parts], [p[:, COLS:] for p in parts]


def spots(hots, inside, whole, base):
    rows = []
    for e in range(ELEMS):
        rows.append(jnp.sum(hots[e] * (inside[e] + base), axis=0, keepdims=True))
        base = base + whole[e]
    return rows


def pack_kernel(me_ref, owner_hbm, local_hbm, coord_hbm, mass_hbm, old_hbm, tracer_hbm, req_ref, away_ref, vals_ref, old_ref, tracer_ref, owner_ref, local_ref, coord_ref, mass_ref, sem):
    pairs = (
        (owner_hbm, owner_ref),
        (local_hbm, local_ref),
        (coord_hbm, coord_ref),
        (mass_hbm, mass_ref),
        (old_hbm, old_ref),
        (tracer_hbm, tracer_ref),
    )
    copies = [pltpu.make_async_copy(src, dst, sem.at[i]) for i, (src, dst) in enumerate(pairs)]
    for copy in copies:
        copy.start()
    me = me_ref[0]
    for copy in copies[:4]:
        copy.wait()
    owner = in_group(owner_ref[...])
    owner = jnp.where(owner == me, -1, owner)
    away_ref[...] = owner
    level = iota((ELEMS, COLS), 1) // NODES
    row = (local_ref[...] * LEVELS + (level + 1)).astype(F32)
    mass = mass_ref[...]
    vals_ref[:ELEMS] = row
    vals_ref[ELEMS : 2 * ELEMS] = coord_ref[0]
    vals_ref[2 * ELEMS : 3 * ELEMS] = coord_ref[1]
    vals_ref[3 * ELEMS :] = jnp.where(owner < 0, mass, 0.0)
    values = (row, coord_ref[0], coord_ref[1], mass)
    hots, inside, whole = ranks(owner)
    slot = (iota((DEVS, COLS), 0) % SLOTS).astype(F32)
    wide = []
    for e, spot in enumerate(spots(hots, inside, whole, jnp.zeros((DEVS, COLS), F32))):
        value = jnp.concatenate([jnp.broadcast_to(v[e : e + 1], (SLOTS, COLS)) for v in values], axis=0)
        wide.append(jnp.where(jnp.broadcast_to(spot, (DEVS, COLS)) == slot, value, 0.0))
    hot = jnp.concatenate(hots, axis=1).astype(BF16)
    high, mid = split2(jnp.concatenate(wide, axis=1))
    req_ref[...] = dot_nt(hot, high) + dot_nt(hot, mid)
    for copy in copies[4:]:
        copy.wait()


def node_constants(n):
    def one(index):
        p0 = jnp.where(index > 0, GLL[0], GLL[1])
        p1 = jnp.where(index > 1, GLL[1], GLL[2])
        p2 = jnp.where(index > 2, GLL[2], GLL[3])
        scale = []
        for i in range(4):
            prod = 1.0
            for j in range(4):
                if j != i:
                    prod *= GLL[i] - GLL[j]
            scale.append(1.0 / prod)
        c = jnp.where(index == 0, scale[0], jnp.where(index == 1, scale[1], jnp.where(index == 2, scale[2], scale[3])))
        return p0, p1, p2, c

    k = iota((NODES, n), 0)
    return one(k // 4), one(k % 4)


def lagrange(x, consts):
    p0, p1, p2, c = consts
    return ((x - p0) * (x - p1)) * ((x - p2) * c)


def evaluate(row, a, b, mass, table, consts):
    n = row.shape[1]
    index = jnp.maximum(row.astype(I32) - 1, 0)
    index8 = jnp.broadcast_to(index, (8, n))
    level8 = index8 % LEVELS
    sub8 = iota((8, n), 0)
    hot = jnp.concatenate([jnp.where(index8 == sub8 + 8 * e, 1.0, 0.0) for e in range(ELEMS)], axis=0).astype(BF16)
    values = dot(table, jnp.concatenate([hot, hot, hot], axis=0))
    w = lagrange(jnp.broadcast_to(a, (NODES, n)), consts[0]) * lagrange(jnp.broadcast_to(b, (NODES, n)), consts[1])
    weights = [jnp.broadcast_to(w[k : k + 1], (8, n)) for k in range(NODES)]
    clipped, highest, lowest = [], [], []
    for t in range(Q // 8):
        v = values[8 * t : 8 * t + 8]
        total, low, high = weights[0] * v, v, v
        for k in range(1, NODES):
            v = values[k * Q + 8 * t : k * Q + 8 * t + 8]
            total = total + weights[k] * v
            low = jnp.minimum(low, v)
            high = jnp.maximum(high, v)
        clipped.append(jnp.minimum(jnp.maximum(total, low), high))
        highest.append(high)
        lowest.append(low)
    mass8 = jnp.broadcast_to(mass, (8, n))
    mh = mass8.astype(BF16).astype(F32)
    mm = mass8 - mh
    mine = level8 == sub8
    by_level = jnp.concatenate([jnp.where(mine, mh, 0.0), jnp.where(mine, mm, 0.0)], axis=0).astype(BF16)
    ch, cm = split2(jnp.concatenate(clipped, axis=0))
    sums = dot_nt(jnp.concatenate([ch, cm], axis=0), by_level)
    mmh = mm.astype(BF16).astype(F32)
    mass3 = jnp.where(sub8 == 0, mh, jnp.where(sub8 == 1, mmh, jnp.where(sub8 == 2, mm - mmh, 0.0)))
    hist = dot_nt(jnp.concatenate([mass3, mass3 * 0.0], axis=0).astype(BF16), hot)
    return clipped, highest, lowest, sums, hist, level8


def spread_terms(clipped, highest, lowest):
    margin = 0.01 + 0.05 * (highest - lowest)
    return highest + margin - clipped, clipped - lowest + margin


def fold(x):
    total = x[:, :LEVELS]
    for e in range(1, ELEMS):
        total = total + x[:, e * LEVELS : (e + 1) * LEVELS]
    return total


def level_sums(sums, hist, low_table, high_table):
    s = sums[:Q] + sums[Q:]
    clip = s[:, :LEVELS] + s[:, LEVELS:]
    mass = hist[0:1] + hist[1:2] + hist[2:3]

    s_low = fold(low_table * mass)
    s_high = fold(high_table * mass)
    margin = 0.01 * fold(jnp.broadcast_to(mass, (Q, mass.shape[1]))) + 0.05 * (s_high - s_low)
    return clip, s_high + margin - clip, clip - s_low + margin


def home_kernel(tracer_ref, old_ref, vals_ref, away_ref, table_ref, bt_ref, part_ref, hot_ref, peer_ref, c_ref, up_ref, down_ref, scratch):
    rows = ELEMS * LEVELS
    node = iota((NODES, COLS), 0)
    column = iota((NODES, COLS), 1)
    wide = jnp.concatenate([jnp.where(column % NODES == node, jnp.broadcast_to(old_ref[e : e + 1, :], (NODES, COLS)), 0.0) for e in range(ELEMS)], axis=1)
    source_of = iota((ELEMS * COLS, rows), 0)
    gather = jnp.where(source_of // NODES == iota((ELEMS * COLS, rows), 1), 1.0, 0.0).astype(BF16)
    old = sum(dot(part, gather) for part in split3(wide))
    natural = tracer_ref[...].reshape(rows, NODES * Q)
    flat = [natural[:, 128 * j : 128 * (j + 1)].T for j in range(NODES * Q // 128)]
    for j, piece in enumerate(flat):
        table_ref[128 * j : 128 * (j + 1), :] = jnp.concatenate(split3(piece), axis=1)
    flat = jnp.concatenate(flat, axis=0)
    source = low = high = None
    for k in range(NODES):
        v = flat[k * Q : (k + 1) * Q]
        term = v * old[k : k + 1, :]
        source = term if source is None else source + term
        low = v if low is None else jnp.minimum(low, v)
        high = v if high is None else jnp.maximum(high, v)
    bt_ref[:Q] = low
    bt_ref[Q:] = high
    consts = node_constants(2 * COLS)
    table = table_ref[...]
    sums, hist = None, None
    for e in range(0, ELEMS, 2):
        args = [jnp.concatenate([vals_ref[v * ELEMS + e : v * ELEMS + e + 1], vals_ref[v * ELEMS + e + 1 : v * ELEMS + e + 2]], axis=1) for v in range(4)]
        clipped, highest, lowest, s, h, _ = evaluate(*args, table, consts)
        sums = s if sums is None else sums + s
        hist = h if hist is None else hist + h
        for i in range(Q // 8):
            up, down = spread_terms(clipped[i], highest[i], lowest[i])
            for j in range(2):
                at = slice((e + j) * Q + 8 * i, (e + j) * Q + 8 * i + 8)
                c_ref[at, :] = clipped[i][:, j * COLS : (j + 1) * COLS]
                up_ref[at, :] = up[:, j * COLS : (j + 1) * COLS]
                down_ref[at, :] = down[:, j * COLS : (j + 1) * COLS]
    clip, up, down = level_sums(sums, hist, low, high)
    pad = jnp.zeros((Q, COLS - 3 * LEVELS), F32)
    part_ref[...] = jnp.concatenate([fold(source) - clip, up, down, pad], axis=1)
    away = away_ref[...]
    hots, inside, whole = ranks(away)
    total = whole[0]
    for e in range(1, ELEMS):
        total = total + whole[e]
    device = iota((DEVS, COLS), 0)
    present = jnp.where(total > 0.0, 1.0, 0.0)
    earlier = jnp.where(iota((DEVS, COLS), 1) < device, 1.0, 0.0).astype(BF16)
    peer = dot(earlier, present.astype(BF16))
    ids = [jnp.sum(jnp.where(peer == float(p), present, 0.0) * device.astype(F32), axis=0, keepdims=True) for p in range(PEERS)]
    named = jnp.sum(present, axis=0, keepdims=True)
    ids = [ids[0]] + [jnp.where(named > float(p), ids[p], ids[0]) for p in range(1, PEERS)]
    peer_ref[...] = jnp.concatenate(ids + [named] * (8 - PEERS), axis=0).astype(I32)
    place = jnp.where(away < 0, -1.0, jnp.concatenate(spots(hots, inside, whole, peer * float(SLOTS)), axis=0))
    scratch[...] = jnp.concatenate([place, jnp.full((COLS - ELEMS, COLS), -1.0, F32)], axis=0).T
    turned = jnp.concatenate([scratch[pl.ds(k, LEVELS, stride=NODES), :] for k in range(NODES)], axis=0)
    lane = iota((COLS, SLOTS * 8), 1).astype(F32)
    for e in range(ELEMS):
        col = jnp.broadcast_to(turned[:, e : e + 1], (COLS, SLOTS * 8))
        hot_ref[e * COLS : (e + 1) * COLS, :] = jnp.where(col == lane, 1.0, 0.0).astype(BF16)


def serve_kernel(me_ref, req_ref, table_ref, part_ref, bt_ref, keep_ref, give_ref, ids_ref, level_ref, c_ref, up_ref, down_ref, dense, tiles):
    req = req_ref[...]
    sub = iota((DEVS, DEVS), 0)
    lane = iota((DEVS, DEVS), 1)
    high, mid = split2(req)
    first = jnp.where(iota((16, DEVS), 1) == 0, 1.0, 0.0).astype(BF16)
    asks = jnp.where(dot_nt(first, high) > 0.0, 1.0, 0.0)
    place = dot(asks.astype(BF16), jnp.where(sub < lane, 1.0, 0.0).astype(BF16))
    count = jnp.sum(asks[0:1]).astype(I32)
    pick = jnp.where(jnp.broadcast_to(place[0:1], (DEVS, DEVS)) == sub.astype(F32), jnp.broadcast_to(asks[0:1], (DEVS, DEVS)), 0.0).astype(BF16)
    dense[...] = dot(pick, high) + dot(pick, mid)
    ids = dot_nt(iota((16, DEVS), 1).astype(F32).astype(BF16), pick)[:8].astype(I32)
    ids = jnp.where(iota((8, DEVS), 1) < count, ids, me_ref[0])
    ids_ref[...] = jnp.where(iota((8, DEVS), 0) == 0, ids, count)
    groups = [dense[pl.ds(i, DEVS // 4, stride=4), :] for i in range(4)]
    block = iota((DEVS // 4, DEVS), 1) // SLOTS
    for v in range(4):
        tile = None
        for i in range(4):
            shift = (i - v) * SLOTS % DEVS
            moved = pltpu.roll(groups[i], shift, 1) if shift else groups[i]
            tile = moved if tile is None else jnp.where(block == i, moved, tile)
        tiles[v] = tile
    consts = node_constants(2 * DEVS)

    def step(u, carry):
        args = [jnp.concatenate([tiles[v, pl.ds(2 * u, 1), :], tiles[v, pl.ds(2 * u + 1, 1), :]], axis=1) for v in range(4)]
        clipped, highest, lowest, s, h, level8 = evaluate(*args, table_ref[...], consts)
        for j in range(2):
            level_ref[pl.ds(pl.multiple_of(16 * u + 8 * j, 8), 8), :] = level8[:, j * DEVS : (j + 1) * DEVS]
        for i in range(Q // 8):
            up, down = spread_terms(clipped[i], highest[i], lowest[i])
            for j in range(2):
                at = pl.ds(pl.multiple_of(2 * Q * u + j * Q + 8 * i, 8), 8)
                c_ref[at, :] = clipped[i][:, j * DEVS : (j + 1) * DEVS]
                up_ref[at, :] = up[:, j * DEVS : (j + 1) * DEVS]
                down_ref[at, :] = down[:, j * DEVS : (j + 1) * DEVS]
        return carry[0] + s, carry[1] + h

    start = (jnp.zeros((2 * Q, 2 * LEVELS), F32), jnp.zeros((16, ELEMS * LEVELS), F32))
    start = step(1, step(0, start))
    sums, hist = lax.fori_loop(2, (count + 7) // 8, step, start)
    clip, up, down = level_sums(sums, hist, bt_ref[:Q, :], bt_ref[Q:, :])
    part = jnp.concatenate([-clip, up, down], axis=1) + part_ref[:, : 3 * LEVELS]
    packed = [part[8 * i : 8 * i + 8] for i in range(Q // 8)]
    packed.append(jnp.zeros((8, COLS - 3 * LEVELS * (Q // 8)), F32))
    packed = jnp.concatenate(packed, axis=1)
    upper = jnp.full((4, COLS), me_ref[0], I32) >= DEVS // 2
    keep_ref[...] = jnp.where(upper, packed[4:], packed[:4])
    give_ref[...] = jnp.where(upper, packed[:4], packed[4:])


def spread_kernel(keep_ref, got_ref, sums_ref):
    half = keep_ref[...] + got_ref[...]
    both = jnp.concatenate([half, half], axis=0)
    for d in range(DEVS // 2):
        sums_ref[8 * d : 8 * d + 8, :] = both


def finish_kernel(ids_ref, tot_ref, level_ref, c_ref, up_ref, down_ref, away_ref, hc_ref, hu_ref, hd_ref, ans_ref, home_ref, scratch):
    halves = []
    for core in range(2):
        at = core * 4 * (DEVS // 2)
        total = tot_ref[at : at + 8, :]
        for d in range(1, DEVS // 4):
            total = total + tot_ref[at + 8 * d : at + 8 * d + 8, :]
        halves.append(total[:4] + total[4:])
    total = jnp.concatenate(halves, axis=0)
    up_total = pltpu.roll(total, COLS - LEVELS, 1)
    down_total = pltpu.roll(total, COLS - 2 * LEVELS, 1)
    lanes = iota((8, COLS), 1)
    real = (lanes < 3 * LEVELS * (Q // 8)) & (lanes % (3 * LEVELS) < LEVELS)
    rise = jnp.where(real, jnp.maximum(total, 0.0) / up_total, 0.0)
    fall = jnp.where(real, jnp.minimum(total, 0.0) / down_total, 0.0)
    coef = [x[:, 24 * i : 24 * i + LEVELS] for x in (rise, fall) for i in range(Q // 8)]
    coef = jnp.concatenate(split3(jnp.concatenate(coef, axis=0)), axis=1)

    def by_level(level8):
        hot = jnp.where(level8 == iota((8, 128), 0), 1.0, 0.0)
        c = dot(coef, jnp.concatenate([hot] * 3, axis=0).astype(BF16))
        return c[:Q], c[Q:]

    block = iota((CHUNK, DEVS), 1) // SLOTS

    def step(t, carry):
        r, f = by_level(level_ref[pl.ds(pl.multiple_of(8 * t, 8), 8), :])
        at = pl.ds(pl.multiple_of(Q * t, 8), Q)
        out = c_ref[at, :] + r * up_ref[at, :] + f * down_ref[at, :]
        parts = [out[CHUNK * b : CHUNK * (b + 1)] for b in range(4)]
        for i in range(4):
            chunk = None
            for b in range(4):
                shift = (b - i) * SLOTS % DEVS
                moved = pltpu.roll(parts[b], shift, 1) if shift else parts[b]
                chunk = moved if chunk is None else jnp.where(block == b, moved, chunk)
            ans_ref[pl.ds(ids_ref[0, 4 * t + i] * CHUNK, CHUNK), :] = chunk
        return carry

    for t in range(3):
        step(t, 0)
    lax.fori_loop(3, (ids_ref[1, 0] + 3) // 4, step, 0)
    r, f = by_level(iota((8, COLS), 1) // NODES)
    for e in range(ELEMS):
        at = slice(e * Q, (e + 1) * Q)
        v = hc_ref[at, :] + r * hu_ref[at, :] + f * hd_ref[at, :]
        v = jnp.where(jnp.broadcast_to(away_ref[e : e + 1, :], (Q, COLS)) < 0, v, 0.0)
        scratch[e] = jnp.concatenate([v, jnp.zeros((COLS - Q, COLS), F32)], axis=0).T
        for k in range(NODES):
            home_ref[e * COLS + 8 * k : e * COLS + 8 * k + 8, :] = scratch[e, pl.ds(k, LEVELS, stride=NODES), :]


def join_kernel(peer_ref, ans_ref, hot_ref, home_ref, out_hbm, out_ref, sem):
    block = iota((CHUNK, 128), 1) // SLOTS
    chunks = [ans_ref[pl.ds(peer_ref[p, 0] * CHUNK, CHUNK), :] for p in range(PEERS)]
    table = []
    for b in range(4):

        def moved(p):
            shift = (p - b) * SLOTS % 128
            return pltpu.roll(chunks[p], shift, 1) if shift else chunks[p]

        near = moved(0)
        for p in range(1, 4):
            near = jnp.where(block == p, moved(p), near)
        table.append(jnp.concatenate([near, jnp.where(block == 0, moved(4), 0.0)], axis=1))
    high, mid = split2(jnp.concatenate(table, axis=0))
    for e in range(ELEMS):
        hot = hot_ref[e * COLS : (e + 1) * COLS, :]
        v = dot_nt(hot, high) + dot_nt(hot, mid) + home_ref[e * COLS : (e + 1) * COLS, :Q]
        out_ref[e] = jnp.concatenate([v[8 * k : 8 * k + 8] for k in range(NODES)], axis=1)
        pltpu.make_async_copy(out_ref.at[e], out_hbm.at[e], sem.at[e]).start()
    for e in range(ELEMS):
        pltpu.make_async_copy(out_ref.at[e], out_hbm.at[e], sem.at[e]).wait()


def body(tracer, old_mass, new_mass, dep_owner, dep_local, dep_coord):
    me = lax.axis_index(GROUP).astype(I32).reshape(1)
    owner = dep_owner.reshape(ELEMS, COLS)
    smem, vmem, hbm = (pl.BlockSpec(memory_space=m) for m in (pltpu.SMEM, pltpu.VMEM, pltpu.HBM))

    def near(*arrays):
        return [pltpu.with_memory_space_constraint(x, pltpu.VMEM) for x in arrays]

    def call(kernel, name, outs, in_specs, scratch, args):
        return pl.pallas_call(
            kernel,
            out_shape=tuple(pltpu.VMEM(shape, dtype) for shape, dtype in outs),
            in_specs=in_specs,
            out_specs=(vmem,) * len(outs),
            scratch_shapes=scratch,
            compiler_params=pltpu.CompilerParams(vmem_limit_bytes=20 << 20),
            name=name,
        )(*args)

    def exchange(x, chunk):
        y = lax.all_to_all(x.reshape((DEVS,) + chunk), GROUP, 0, 0, tiled=True)
        return y.reshape(x.shape)

    req, away, vals, old, near_tracer = call(
        pack_kernel,
        "pack",
        (
            ((DEVS, COLS), F32),
            ((ELEMS, COLS), I32),
            ((4 * ELEMS, COLS), F32),
            ((ELEMS, COLS), F32),
            (tracer.shape, F32),
        ),
        [smem] + [hbm] * 6,
        [
            pltpu.VMEM((ELEMS, COLS), I32),
            pltpu.VMEM((ELEMS, COLS), I32),
            pltpu.VMEM((2, ELEMS, COLS), F32),
            pltpu.VMEM((ELEMS, COLS), F32),
            pltpu.SemaphoreType.DMA((6,)),
        ],
        [me] + [pltpu.with_memory_space_constraint(x, pltpu.HBM) for x in (owner, dep_local, dep_coord, new_mass, old_mass, tracer)],
    )
    asked = exchange(req, (1, COLS))
    table, bt, part, hot, peer, hc, hu, hd = call(
        home_kernel,
        "home",
        (
            ((NODES * Q, 3 * ELEMS * LEVELS), BF16),
            ((2 * Q, ELEMS * LEVELS), F32),
            ((Q, COLS), F32),
            ((ELEMS * COLS, SLOTS * 8), BF16),
            ((8, COLS), I32),
        )
        + (((ELEMS * Q, COLS), F32),) * 3,
        [vmem] * 4,
        [pltpu.VMEM((COLS, COLS), F32)],
        near(near_tracer, old, vals, away),
    )
    keep, give, ids, level, c, up, down = call(
        serve_kernel,
        "serve",
        (((4, COLS), F32), ((4, COLS), F32), ((8, DEVS), I32), ((2 * DEVS, DEVS), I32)) + (((SLOTS * Q, DEVS), F32),) * 3,
        [smem] + [vmem] * 4,
        [pltpu.VMEM((DEVS, DEVS), F32), pltpu.VMEM((4, DEVS // 4, DEVS), F32)],
        [me] + near(asked, table, part, bt),
    )
    given = lax.ppermute(give, "core", [(0, 1), (1, 0)])
    (sums,) = call(spread_kernel, "spread", (((4 * DEVS, COLS), F32),), [vmem] * 2, [], near(keep, given))
    totals = exchange(sums, (4, COLS))
    ans, home = call(
        finish_kernel,
        "finish",
        (((DEVS * CHUNK, 128), F32), ((ELEMS * COLS, 128), F32)),
        [smem] + [vmem] * 9,
        [pltpu.VMEM((ELEMS, COLS, 128), F32)],
        [ids] + near(totals, level, c, up, down, away, hc, hu, hd),
    )
    got = exchange(ans, (1, SLOTS * Q))
    return pl.pallas_call(
        join_kernel,
        out_shape=jax.ShapeDtypeStruct((ELEMS, LEVELS, NODES * Q), F32),
        in_specs=[smem] + [vmem] * 3,
        out_specs=hbm,
        scratch_shapes=[pltpu.VMEM((ELEMS, LEVELS, NODES * Q), F32), pltpu.SemaphoreType.DMA((ELEMS,))],
        compiler_params=pltpu.CompilerParams(vmem_limit_bytes=20 << 20),
        name="join",
    )(peer, *near(got, hot, home))


def solution(mesh):
    torus = Mesh(mesh.devices.reshape(4, 4, 4, 2), AXES)
    placed = (
        P(AXES, None, None),
        P(AXES, None),
        P(AXES, None),
        P(AXES, None, None),
        P(AXES, None),
        P(None, AXES, None),
    )
    return jax.shard_map(body, mesh=torus, in_specs=placed, out_specs=P(AXES, None, None), check_vma=False)
```

```python
import jax
import jax.numpy as jnp
from jax import lax
from jax.experimental import pallas as pl
from jax.experimental.pallas import tpu as pltpu
from jax.sharding import Mesh
from jax.sharding import PartitionSpec as P

AXES = ("x", "y", "z", "core")
GROUP = ("core", "z", "y", "x")
GLL = (-1.0, -0.4472135954999579, 0.4472135954999579, 1.0)
DEVS = 128
ELEMS = 8
LEVELS = 8
NODES = 16
Q = 40
SLOTS = 32
PEERS = 5
COLS = LEVELS * NODES
CHUNK = SLOTS * Q // 128
F32, BF16, I32 = jnp.float32, jnp.bfloat16, jnp.int32
NT = (((1,), (1,)), ((), ()))


def iota(shape, dim):
    return lax.broadcasted_iota(I32, shape, dim)


def in_group(device):
    core, z, y, x = device % 2, device // 2 % 4, device // 8 % 4, device // 32
    return core * 64 + z * 16 + y * 4 + x


def dot(a, b):
    return jnp.dot(a, b, preferred_element_type=F32)


def dot_nt(a, b):
    return lax.dot_general(a, b, NT, preferred_element_type=F32)


def split2(x):
    high = x.astype(BF16)
    return high, (x - high.astype(F32)).astype(BF16)


def split3(x):
    high = x.astype(BF16)
    rest = x - high.astype(F32)
    mid = rest.astype(BF16)
    return high, mid, (rest - mid.astype(F32)).astype(BF16)


def ranks(owner):
    sub = iota((DEVS, COLS), 0)
    before = jnp.where(sub < iota((DEVS, COLS), 1), 1.0, 0.0).astype(BF16)
    counter = jnp.concatenate([before, jnp.ones((COLS, COLS), BF16)], axis=1)
    hots = [jnp.where(jnp.broadcast_to(owner[e : e + 1], (DEVS, COLS)) == sub, 1.0, 0.0) for e in range(ELEMS)]
    counts = dot(jnp.concatenate(hots, axis=0).astype(BF16), counter)
    parts = [counts[e * DEVS : (e + 1) * DEVS] for e in range(ELEMS)]
    return hots, [p[:, :COLS] for p in parts], [p[:, COLS:] for p in parts]


def spots(hots, inside, whole, base):
    rows = []
    for e in range(ELEMS):
        rows.append(jnp.sum(hots[e] * (inside[e] + base), axis=0, keepdims=True))
        base = base + whole[e]
    return rows


def pack_kernel(me_ref, owner_hbm, local_hbm, coord_hbm, mass_hbm, old_hbm, tracer_hbm, req_ref, away_ref, vals_ref, old_ref, tracer_ref, owner_ref, local_ref, coord_ref, mass_ref, sem):
    pairs = (
        (owner_hbm, owner_ref),
        (local_hbm, local_ref),
        (coord_hbm, coord_ref),
        (mass_hbm, mass_ref),
        (old_hbm, old_ref),
        (tracer_hbm, tracer_ref),
    )
    copies = [pltpu.make_async_copy(src, dst, sem.at[i]) for i, (src, dst) in enumerate(pairs)]
    for copy in copies:
        copy.start()
    me = me_ref[0]
    for copy in copies[:4]:
        copy.wait()
    owner = in_group(owner_ref[...])
    owner = jnp.where(owner == me, -1, owner)
    away_ref[...] = owner
    level = iota((ELEMS, COLS), 1) // NODES
    row = (local_ref[...] * LEVELS + (level + 1)).astype(F32)
    mass = mass_ref[...]
    vals_ref[:ELEMS] = row
    vals_ref[ELEMS : 2 * ELEMS] = coord_ref[0]
    vals_ref[2 * ELEMS : 3 * ELEMS] = coord_ref[1]
    vals_ref[3 * ELEMS :] = jnp.where(owner < 0, mass, 0.0)
    values = (row, coord_ref[0], coord_ref[1], mass)
    hots, inside, whole = ranks(owner)
    slot = (iota((DEVS, COLS), 0) % SLOTS).astype(F32)
    wide = []
    for e, spot in enumerate(spots(hots, inside, whole, jnp.zeros((DEVS, COLS), F32))):
        value = jnp.concatenate([jnp.broadcast_to(v[e : e + 1], (SLOTS, COLS)) for v in values], axis=0)
        wide.append(jnp.where(jnp.broadcast_to(spot, (DEVS, COLS)) == slot, value, 0.0))
    hot = jnp.concatenate(hots, axis=1).astype(BF16)
    high, mid = split2(jnp.concatenate(wide, axis=1))
    req_ref[...] = dot_nt(hot, high) + dot_nt(hot, mid)
    for copy in copies[4:]:
        copy.wait()


def node_constants(n):
    def one(index):
        p0 = jnp.where(index > 0, GLL[0], GLL[1])
        p1 = jnp.where(index > 1, GLL[1], GLL[2])
        p2 = jnp.where(index > 2, GLL[2], GLL[3])
        scale = []
        for i in range(4):
            prod = 1.0
            for j in range(4):
                if j != i:
                    prod *= GLL[i] - GLL[j]
            scale.append(1.0 / prod)
        c = jnp.where(index == 0, scale[0], jnp.where(index == 1, scale[1], jnp.where(index == 2, scale[2], scale[3])))
        return p0, p1, p2, c

    k = iota((NODES, n), 0)
    return one(k // 4), one(k % 4)


def lagrange(x, consts):
    p0, p1, p2, c = consts
    return ((x - p0) * (x - p1)) * ((x - p2) * c)


def evaluate(row, a, b, mass, table, consts):
    n = row.shape[1]
    index = jnp.maximum(row.astype(I32) - 1, 0)
    index8 = jnp.broadcast_to(index, (8, n))
    level8 = index8 % LEVELS
    sub8 = iota((8, n), 0)
    hot = jnp.concatenate([jnp.where(index8 == sub8 + 8 * e, 1.0, 0.0) for e in range(ELEMS)], axis=0).astype(BF16)
    values = dot(table, jnp.concatenate([hot, hot, hot], axis=0))
    w = lagrange(jnp.broadcast_to(a, (NODES, n)), consts[0]) * lagrange(jnp.broadcast_to(b, (NODES, n)), consts[1])
    weights = [jnp.broadcast_to(w[k : k + 1], (8, n)) for k in range(NODES)]
    clipped, highest, lowest = [], [], []
    for t in range(Q // 8):
        v = values[8 * t : 8 * t + 8]
        total, low, high = weights[0] * v, v, v
        for k in range(1, NODES):
            v = values[k * Q + 8 * t : k * Q + 8 * t + 8]
            total = total + weights[k] * v
            low = jnp.minimum(low, v)
            high = jnp.maximum(high, v)
        clipped.append(jnp.minimum(jnp.maximum(total, low), high))
        highest.append(high)
        lowest.append(low)
    mass8 = jnp.broadcast_to(mass, (8, n))
    mh = mass8.astype(BF16).astype(F32)
    mm = mass8 - mh
    mine = level8 == sub8
    by_level = jnp.concatenate([jnp.where(mine, mh, 0.0), jnp.where(mine, mm, 0.0)], axis=0).astype(BF16)
    ch, cm = split2(jnp.concatenate(clipped, axis=0))
    sums = dot_nt(jnp.concatenate([ch, cm], axis=0), by_level)
    mmh = mm.astype(BF16).astype(F32)
    mass3 = jnp.where(sub8 == 0, mh, jnp.where(sub8 == 1, mmh, jnp.where(sub8 == 2, mm - mmh, 0.0)))
    hist = dot_nt(jnp.concatenate([mass3, mass3 * 0.0], axis=0).astype(BF16), hot)
    return clipped, highest, lowest, sums, hist, level8


def spread_terms(clipped, highest, lowest):
    margin = 0.01 + 0.05 * (highest - lowest)
    return highest + margin - clipped, clipped - lowest + margin


def fold(x):
    total = x[:, :LEVELS]
    for e in range(1, ELEMS):
        total = total + x[:, e * LEVELS : (e + 1) * LEVELS]
    return total


def level_sums(sums, hist, low_table, high_table):
    s = sums[:Q] + sums[Q:]
    clip = s[:, :LEVELS] + s[:, LEVELS:]
    mass = hist[0:1] + hist[1:2] + hist[2:3]

    s_low = fold(low_table * mass)
    s_high = fold(high_table * mass)
    margin = 0.01 * fold(jnp.broadcast_to(mass, (Q, mass.shape[1]))) + 0.05 * (s_high - s_low)
    return clip, s_high + margin - clip, clip - s_low + margin


def home_kernel(tracer_ref, old_ref, vals_ref, away_ref, table_ref, bt_ref, part_ref, hot_ref, peer_ref, c_ref, up_ref, down_ref, scratch):
    rows = ELEMS * LEVELS
    node = iota((NODES, COLS), 0)
    column = iota((NODES, COLS), 1)
    wide = jnp.concatenate([jnp.where(column % NODES == node, jnp.broadcast_to(old_ref[e : e + 1, :], (NODES, COLS)), 0.0) for e in range(ELEMS)], axis=1)
    source_of = iota((ELEMS * COLS, rows), 0)
    gather = jnp.where(source_of // NODES == iota((ELEMS * COLS, rows), 1), 1.0, 0.0).astype(BF16)
    old = sum(dot(part, gather) for part in split3(wide))
    natural = tracer_ref[...].reshape(rows, NODES * Q)
    flat = [natural[:, 128 * j : 128 * (j + 1)].T for j in range(NODES * Q // 128)]
    for j, piece in enumerate(flat):
        table_ref[128 * j : 128 * (j + 1), :] = jnp.concatenate(split3(piece), axis=1)
    flat = jnp.concatenate(flat, axis=0)
    source = low = high = None
    for k in range(NODES):
        v = flat[k * Q : (k + 1) * Q]
        term = v * old[k : k + 1, :]
        source = term if source is None else source + term
        low = v if low is None else jnp.minimum(low, v)
        high = v if high is None else jnp.maximum(high, v)
    bt_ref[:Q] = low
    bt_ref[Q:] = high
    consts = node_constants(2 * COLS)
    table = table_ref[...]
    sums, hist = None, None
    for e in range(0, ELEMS, 2):
        args = [jnp.concatenate([vals_ref[v * ELEMS + e : v * ELEMS + e + 1], vals_ref[v * ELEMS + e + 1 : v * ELEMS + e + 2]], axis=1) for v in range(4)]
        clipped, highest, lowest, s, h, _ = evaluate(*args, table, consts)
        sums = s if sums is None else sums + s
        hist = h if hist is None else hist + h
        for i in range(Q // 8):
            up, down = spread_terms(clipped[i], highest[i], lowest[i])
            for j in range(2):
                at = slice((e + j) * Q + 8 * i, (e + j) * Q + 8 * i + 8)
                c_ref[at, :] = clipped[i][:, j * COLS : (j + 1) * COLS]
                up_ref[at, :] = up[:, j * COLS : (j + 1) * COLS]
                down_ref[at, :] = down[:, j * COLS : (j + 1) * COLS]
    clip, up, down = level_sums(sums, hist, low, high)
    pad = jnp.zeros((Q, COLS - 3 * LEVELS), F32)
    part_ref[...] = jnp.concatenate([fold(source) - clip, up, down, pad], axis=1)
    away = away_ref[...]
    hots, inside, whole = ranks(away)
    total = whole[0]
    for e in range(1, ELEMS):
        total = total + whole[e]
    device = iota((DEVS, COLS), 0)
    present = jnp.where(total > 0.0, 1.0, 0.0)
    earlier = jnp.where(iota((DEVS, COLS), 1) < device, 1.0, 0.0).astype(BF16)
    peer = dot(earlier, present.astype(BF16))
    ids = [jnp.sum(jnp.where(peer == float(p), present, 0.0) * device.astype(F32), axis=0, keepdims=True) for p in range(PEERS)]
    named = jnp.sum(present, axis=0, keepdims=True)
    ids = [ids[0]] + [jnp.where(named > float(p), ids[p], ids[0]) for p in range(1, PEERS)]
    peer_ref[...] = jnp.concatenate(ids + [named] * (8 - PEERS), axis=0).astype(I32)
    place = jnp.where(away < 0, -1.0, jnp.concatenate(spots(hots, inside, whole, peer * float(SLOTS)), axis=0))
    scratch[...] = jnp.concatenate([place, jnp.full((COLS - ELEMS, COLS), -1.0, F32)], axis=0).T
    turned = jnp.concatenate([scratch[pl.ds(k, LEVELS, stride=NODES), :] for k in range(NODES)], axis=0)
    lane = iota((COLS, SLOTS * 8), 1).astype(F32)
    for e in range(ELEMS):
        col = jnp.broadcast_to(turned[:, e : e + 1], (COLS, SLOTS * 8))
        hot_ref[e * COLS : (e + 1) * COLS, :] = jnp.where(col == lane, 1.0, 0.0).astype(BF16)


def serve_kernel(me_ref, req_ref, table_ref, part_ref, bt_ref, keep_ref, give_ref, ids_ref, level_ref, c_ref, up_ref, down_ref, dense, tiles):
    req = req_ref[...]
    sub = iota((DEVS, DEVS), 0)
    lane = iota((DEVS, DEVS), 1)
    high, mid = split2(req)
    first = jnp.where(iota((16, DEVS), 1) == 0, 1.0, 0.0).astype(BF16)
    asks = jnp.where(dot_nt(first, high) > 0.0, 1.0, 0.0)
    place = dot(asks.astype(BF16), jnp.where(sub < lane, 1.0, 0.0).astype(BF16))
    count = jnp.sum(asks[0:1]).astype(I32)
    pick = jnp.where(jnp.broadcast_to(place[0:1], (DEVS, DEVS)) == sub.astype(F32), jnp.broadcast_to(asks[0:1], (DEVS, DEVS)), 0.0).astype(BF16)
    dense[...] = dot(pick, high) + dot(pick, mid)
    ids = dot_nt(iota((16, DEVS), 1).astype(F32).astype(BF16), pick)[:8].astype(I32)
    ids = jnp.where(iota((8, DEVS), 1) < count, ids, me_ref[0])
    ids_ref[...] = jnp.where(iota((8, DEVS), 0) == 0, ids, count)
    groups = [dense[pl.ds(i, DEVS // 4, stride=4), :] for i in range(4)]
    block = iota((DEVS // 4, DEVS), 1) // SLOTS
    for v in range(4):
        tile = None
        for i in range(4):
            shift = (i - v) * SLOTS % DEVS
            moved = pltpu.roll(groups[i], shift, 1) if shift else groups[i]
            tile = moved if tile is None else jnp.where(block == i, moved, tile)
        tiles[v] = tile
    consts = node_constants(2 * DEVS)

    def step(u, carry):
        args = [jnp.concatenate([tiles[v, pl.ds(2 * u, 1), :], tiles[v, pl.ds(2 * u + 1, 1), :]], axis=1) for v in range(4)]
        clipped, highest, lowest, s, h, level8 = evaluate(*args, table_ref[...], consts)
        for j in range(2):
            level_ref[pl.ds(pl.multiple_of(16 * u + 8 * j, 8), 8), :] = level8[:, j * DEVS : (j + 1) * DEVS]
        for i in range(Q // 8):
            up, down = spread_terms(clipped[i], highest[i], lowest[i])
            for j in range(2):
                at = pl.ds(pl.multiple_of(2 * Q * u + j * Q + 8 * i, 8), 8)
                c_ref[at, :] = clipped[i][:, j * DEVS : (j + 1) * DEVS]
                up_ref[at, :] = up[:, j * DEVS : (j + 1) * DEVS]
                down_ref[at, :] = down[:, j * DEVS : (j + 1) * DEVS]
        return carry[0] + s, carry[1] + h

    start = (jnp.zeros((2 * Q, 2 * LEVELS), F32), jnp.zeros((16, ELEMS * LEVELS), F32))
    start = step(1, step(0, start))
    sums, hist = lax.fori_loop(2, (count + 7) // 8, step, start)
    clip, up, down = level_sums(sums, hist, bt_ref[:Q, :], bt_ref[Q:, :])
    part = jnp.concatenate([-clip, up, down], axis=1) + part_ref[:, : 3 * LEVELS]
    packed = [part[8 * i : 8 * i + 8] for i in range(Q // 8)]
    packed.append(jnp.zeros((8, COLS - 3 * LEVELS * (Q // 8)), F32))
    packed = jnp.concatenate(packed, axis=1)
    upper = jnp.full((4, COLS), me_ref[0], I32) >= DEVS // 2
    keep_ref[...] = jnp.where(upper, packed[4:], packed[:4])
    give_ref[...] = jnp.where(upper, packed[:4], packed[4:])


def spread_kernel(keep_ref, got_ref, sums_ref):
    half = keep_ref[...] + got_ref[...]
    both = jnp.concatenate([half, half], axis=0)
    for d in range(DEVS // 2):
        sums_ref[8 * d : 8 * d + 8, :] = both


def finish_kernel(ids_ref, tot_ref, level_ref, c_ref, up_ref, down_ref, away_ref, hc_ref, hu_ref, hd_ref, ans_ref, home_ref, scratch, later, sem):
    halves = []
    for core in range(2):
        at = core * 4 * (DEVS // 2)
        total = tot_ref[at : at + 8, :]
        for d in range(1, DEVS // 4):
            total = total + tot_ref[at + 8 * d : at + 8 * d + 8, :]
        halves.append(total[:4] + total[4:])
    total = jnp.concatenate(halves, axis=0)
    up_total = pltpu.roll(total, COLS - LEVELS, 1)
    down_total = pltpu.roll(total, COLS - 2 * LEVELS, 1)
    lanes = iota((8, COLS), 1)
    real = (lanes < 3 * LEVELS * (Q // 8)) & (lanes % (3 * LEVELS) < LEVELS)
    rise = jnp.where(real, jnp.maximum(total, 0.0) / up_total, 0.0)
    fall = jnp.where(real, jnp.minimum(total, 0.0) / down_total, 0.0)
    coef = [x[:, 24 * i : 24 * i + LEVELS] for x in (rise, fall) for i in range(Q // 8)]
    coef = jnp.concatenate(split3(jnp.concatenate(coef, axis=0)), axis=1)

    def by_level(level8):
        hot = jnp.where(level8 == iota((8, 128), 0), 1.0, 0.0)
        c = dot(coef, jnp.concatenate([hot] * 3, axis=0).astype(BF16))
        return c[:Q], c[Q:]

    block = iota((CHUNK, DEVS), 1) // SLOTS

    first = ids_ref[...]

    def step(t, id_of):
        r, f = by_level(level_ref[pl.ds(pl.multiple_of(8 * t, 8), 8), :])
        at = pl.ds(pl.multiple_of(Q * t, 8), Q)
        out = c_ref[at, :] + r * up_ref[at, :] + f * down_ref[at, :]
        parts = [out[CHUNK * b : CHUNK * (b + 1)] for b in range(4)]
        for i in range(4):
            chunk = None
            for b in range(4):
                shift = (b - i) * SLOTS % DEVS
                moved = pltpu.roll(parts[b], shift, 1) if shift else parts[b]
                chunk = moved if chunk is None else jnp.where(block == b, moved, chunk)
            ans_ref[pl.ds(id_of(4 * t + i) * CHUNK, CHUNK), :] = chunk

    for t in range(3):
        step(t, lambda i: first[0, i])
    count = first[1, 0]

    @pl.when(count > 12)
    def _():
        copy = pltpu.make_async_copy(ids_ref, later, sem)
        copy.start()
        copy.wait()

        def more(t, carry):
            step(t, lambda i: later[0, i])
            return carry

        lax.fori_loop(3, (count + 3) // 4, more, 0)

    r, f = by_level(iota((8, COLS), 1) // NODES)
    for e in range(ELEMS):
        at = slice(e * Q, (e + 1) * Q)
        v = hc_ref[at, :] + r * hu_ref[at, :] + f * hd_ref[at, :]
        v = jnp.where(jnp.broadcast_to(away_ref[e : e + 1, :], (Q, COLS)) < 0, v, 0.0)
        scratch[e] = jnp.concatenate([v, jnp.zeros((COLS - Q, COLS), F32)], axis=0).T
        for k in range(NODES):
            home_ref[e * COLS + 8 * k : e * COLS + 8 * k + 8, :] = scratch[e, pl.ds(k, LEVELS, stride=NODES), :]


def join_kernel(peer_ref, ans_ref, hot_ref, home_ref, out_hbm, out_ref, sem):
    block = iota((CHUNK, 128), 1) // SLOTS
    peers = peer_ref[...]
    chunks = [ans_ref[pl.ds(peers[p, 0] * CHUNK, CHUNK), :] for p in range(PEERS)]
    table = []
    for b in range(4):

        def moved(p):
            shift = (p - b) * SLOTS % 128
            return pltpu.roll(chunks[p], shift, 1) if shift else chunks[p]

        near = moved(0)
        for p in range(1, 4):
            near = jnp.where(block == p, moved(p), near)
        table.append(jnp.concatenate([near, jnp.where(block == 0, moved(4), 0.0)], axis=1))
    high, mid = split2(jnp.concatenate(table, axis=0))
    for e in range(ELEMS):
        hot = hot_ref[e * COLS : (e + 1) * COLS, :]
        v = dot_nt(hot, high) + dot_nt(hot, mid) + home_ref[e * COLS : (e + 1) * COLS, :Q]
        out_ref[e] = jnp.concatenate([v[8 * k : 8 * k + 8] for k in range(NODES)], axis=1)
        pltpu.make_async_copy(out_ref.at[e], out_hbm.at[e], sem.at[e]).start()
    for e in range(ELEMS):
        pltpu.make_async_copy(out_ref.at[e], out_hbm.at[e], sem.at[e]).wait()


def body(tracer, old_mass, new_mass, dep_owner, dep_local, dep_coord):
    me = lax.axis_index(GROUP).astype(I32).reshape(1)
    owner = dep_owner.reshape(ELEMS, COLS)
    smem, vmem, hbm = (pl.BlockSpec(memory_space=m) for m in (pltpu.SMEM, pltpu.VMEM, pltpu.HBM))

    def near(*arrays):
        return [pltpu.with_memory_space_constraint(x, pltpu.VMEM) for x in arrays]

    def call(kernel, name, outs, in_specs, scratch, args):
        return pl.pallas_call(
            kernel,
            out_shape=tuple(pltpu.VMEM(shape, dtype) for shape, dtype in outs),
            in_specs=in_specs,
            out_specs=(vmem,) * len(outs),
            scratch_shapes=scratch,
            compiler_params=pltpu.CompilerParams(vmem_limit_bytes=20 << 20),
            name=name,
        )(*args)

    def exchange(x, chunk):
        y = lax.all_to_all(x.reshape((DEVS,) + chunk), GROUP, 0, 0, tiled=True)
        return y.reshape(x.shape)

    req, away, vals, old, near_tracer = call(
        pack_kernel,
        "pack",
        (
            ((DEVS, COLS), F32),
            ((ELEMS, COLS), I32),
            ((4 * ELEMS, COLS), F32),
            ((ELEMS, COLS), F32),
            (tracer.shape, F32),
        ),
        [smem] + [hbm] * 6,
        [
            pltpu.VMEM((ELEMS, COLS), I32),
            pltpu.VMEM((ELEMS, COLS), I32),
            pltpu.VMEM((2, ELEMS, COLS), F32),
            pltpu.VMEM((ELEMS, COLS), F32),
            pltpu.SemaphoreType.DMA((6,)),
        ],
        [me] + [pltpu.with_memory_space_constraint(x, pltpu.HBM) for x in (owner, dep_local, dep_coord, new_mass, old_mass, tracer)],
    )
    asked = exchange(req, (1, COLS))
    table, bt, part, hot, peer, hc, hu, hd = call(
        home_kernel,
        "home",
        (
            ((NODES * Q, 3 * ELEMS * LEVELS), BF16),
            ((2 * Q, ELEMS * LEVELS), F32),
            ((Q, COLS), F32),
            ((ELEMS * COLS, SLOTS * 8), BF16),
            ((8, COLS), I32),
        )
        + (((ELEMS * Q, COLS), F32),) * 3,
        [vmem] * 4,
        [pltpu.VMEM((COLS, COLS), F32)],
        near(near_tracer, old, vals, away),
    )
    keep, give, ids, level, c, up, down = call(
        serve_kernel,
        "serve",
        (((4, COLS), F32), ((4, COLS), F32), ((8, DEVS), I32), ((2 * DEVS, DEVS), I32)) + (((SLOTS * Q, DEVS), F32),) * 3,
        [smem] + [vmem] * 4,
        [pltpu.VMEM((DEVS, DEVS), F32), pltpu.VMEM((4, DEVS // 4, DEVS), F32)],
        [me] + near(asked, table, part, bt),
    )
    given = lax.ppermute(give, "core", [(0, 1), (1, 0)])
    (sums,) = call(spread_kernel, "spread", (((4 * DEVS, COLS), F32),), [vmem] * 2, [], near(keep, given))
    totals = exchange(sums, (4, COLS))
    ans, home = call(
        finish_kernel,
        "finish",
        (((DEVS * CHUNK, 128), F32), ((ELEMS * COLS, 128), F32)),
        [vmem] * 10,
        [pltpu.VMEM((ELEMS, COLS, 128), F32), pltpu.SMEM((8, DEVS), I32), pltpu.SemaphoreType.DMA],
        near(ids, totals, level, c, up, down, away, hc, hu, hd),
    )
    got = exchange(ans, (1, SLOTS * Q))
    return pl.pallas_call(
        join_kernel,
        out_shape=jax.ShapeDtypeStruct((ELEMS, LEVELS, NODES * Q), F32),
        in_specs=[vmem] * 4,
        out_specs=hbm,
        scratch_shapes=[pltpu.VMEM((ELEMS, LEVELS, NODES * Q), F32), pltpu.SemaphoreType.DMA((ELEMS,))],
        compiler_params=pltpu.CompilerParams(vmem_limit_bytes=20 << 20),
        name="join",
    )(*near(peer, got, hot, home))


def solution(mesh):
    torus = Mesh(mesh.devices.reshape(4, 4, 4, 2), AXES)
    placed = (
        P(AXES, None, None),
        P(AXES, None),
        P(AXES, None),
        P(AXES, None, None),
        P(AXES, None),
        P(None, AXES, None),
    )
    return jax.shard_map(body, mesh=torus, in_specs=placed, out_specs=P(AXES, None, None), check_vma=False)
```

```python
import jax
import jax.numpy as jnp
from jax import lax
from jax.experimental import pallas as pl
from jax.experimental.pallas import tpu as pltpu
from jax.sharding import Mesh
from jax.sharding import PartitionSpec as P

AXES = ("x", "y", "z", "core")
GROUP = ("core", "z", "y", "x")
GLL = (-1.0, -0.4472135954999579, 0.4472135954999579, 1.0)
DEVS = 128
ELEMS = 8
LEVELS = 8
NODES = 16
Q = 40
SLOTS = 32
PEERS = 5
COLS = LEVELS * NODES
CHUNK = SLOTS * Q // 128
F32, BF16, I32 = jnp.float32, jnp.bfloat16, jnp.int32
NT = (((1,), (1,)), ((), ()))


def iota(shape, dim):
    return lax.broadcasted_iota(I32, shape, dim)


def in_group(device):
    core, z, y, x = device % 2, device // 2 % 4, device // 8 % 4, device // 32
    return core * 64 + z * 16 + y * 4 + x


def dot(a, b):
    return jnp.dot(a, b, preferred_element_type=F32)


def dot_nt(a, b):
    return lax.dot_general(a, b, NT, preferred_element_type=F32)


def split2(x):
    high = x.astype(BF16)
    return high, (x - high.astype(F32)).astype(BF16)


def split3(x):
    high = x.astype(BF16)
    rest = x - high.astype(F32)
    mid = rest.astype(BF16)
    return high, mid, (rest - mid.astype(F32)).astype(BF16)


def ranks(owner):
    sub = iota((DEVS, COLS), 0)
    before = jnp.where(sub < iota((DEVS, COLS), 1), 1.0, 0.0).astype(BF16)
    counter = jnp.concatenate([before, jnp.ones((COLS, COLS), BF16)], axis=1)
    hots = [jnp.where(jnp.broadcast_to(owner[e : e + 1], (DEVS, COLS)) == sub, 1.0, 0.0) for e in range(ELEMS)]
    counts = dot(jnp.concatenate(hots, axis=0).astype(BF16), counter)
    parts = [counts[e * DEVS : (e + 1) * DEVS] for e in range(ELEMS)]
    return hots, [p[:, :COLS] for p in parts], [p[:, COLS:] for p in parts]


def spots(hots, inside, whole, base):
    rows = []
    for e in range(ELEMS):
        rows.append(jnp.sum(hots[e] * (inside[e] + base), axis=0, keepdims=True))
        base = base + whole[e]
    return rows


def pack_kernel(me_ref, owner_hbm, local_hbm, coord_hbm, mass_hbm, old_hbm, tracer_hbm, req_ref, away_ref, vals_ref, old_ref, tracer_ref, owner_ref, local_ref, coord_ref, mass_ref, sem):
    pairs = (
        (owner_hbm, owner_ref),
        (local_hbm, local_ref),
        (coord_hbm, coord_ref),
        (mass_hbm, mass_ref),
        (old_hbm, old_ref),
        (tracer_hbm, tracer_ref),
    )
    copies = [pltpu.make_async_copy(src, dst, sem.at[i]) for i, (src, dst) in enumerate(pairs)]
    for copy in copies:
        copy.start()
    me = me_ref[0]
    for copy in copies[:4]:
        copy.wait()
    owner = in_group(owner_ref[...])
    owner = jnp.where(owner == me, -1, owner)
    away_ref[...] = owner
    level = iota((ELEMS, COLS), 1) // NODES
    row = (local_ref[...] * LEVELS + (level + 1)).astype(F32)
    mass = mass_ref[...]
    vals_ref[:ELEMS] = row
    vals_ref[ELEMS : 2 * ELEMS] = coord_ref[0]
    vals_ref[2 * ELEMS : 3 * ELEMS] = coord_ref[1]
    vals_ref[3 * ELEMS :] = jnp.where(owner < 0, mass, 0.0)
    values = (row, coord_ref[0], coord_ref[1], mass)
    hots, inside, whole = ranks(owner)
    slot = (iota((DEVS, COLS), 0) % SLOTS).astype(F32)
    wide = []
    for e, spot in enumerate(spots(hots, inside, whole, jnp.zeros((DEVS, COLS), F32))):
        value = jnp.concatenate([jnp.broadcast_to(v[e : e + 1], (SLOTS, COLS)) for v in values], axis=0)
        wide.append(jnp.where(jnp.broadcast_to(spot, (DEVS, COLS)) == slot, value, 0.0))
    hot = jnp.concatenate(hots, axis=1).astype(BF16)
    high, mid = split2(jnp.concatenate(wide, axis=1))
    req_ref[...] = dot_nt(hot, high) + dot_nt(hot, mid)
    for copy in copies[4:]:
        copy.wait()


def node_constants(n):
    def one(index):
        p0 = jnp.where(index > 0, GLL[0], GLL[1])
        p1 = jnp.where(index > 1, GLL[1], GLL[2])
        p2 = jnp.where(index > 2, GLL[2], GLL[3])
        scale = []
        for i in range(4):
            prod = 1.0
            for j in range(4):
                if j != i:
                    prod *= GLL[i] - GLL[j]
            scale.append(1.0 / prod)
        c = jnp.where(index == 0, scale[0], jnp.where(index == 1, scale[1], jnp.where(index == 2, scale[2], scale[3])))
        return p0, p1, p2, c

    k = iota((NODES, n), 0)
    return one(k // 4), one(k % 4)


def lagrange(x, consts):
    p0, p1, p2, c = consts
    return ((x - p0) * (x - p1)) * ((x - p2) * c)


def evaluate(row, a, b, mass, table, consts):
    n = row.shape[1]
    index = jnp.maximum(row.astype(I32) - 1, 0)
    index8 = jnp.broadcast_to(index, (8, n))
    level8 = index8 % LEVELS
    sub8 = iota((8, n), 0)
    hot = jnp.concatenate([jnp.where(index8 == sub8 + 8 * e, 1.0, 0.0) for e in range(ELEMS)], axis=0).astype(BF16)
    values = dot(table, jnp.concatenate([hot, hot, hot], axis=0))
    w = lagrange(jnp.broadcast_to(a, (NODES, n)), consts[0]) * lagrange(jnp.broadcast_to(b, (NODES, n)), consts[1])
    weights = [jnp.broadcast_to(w[k : k + 1], (8, n)) for k in range(NODES)]
    clipped, highest, lowest = [], [], []
    for t in range(Q // 8):
        v = values[8 * t : 8 * t + 8]
        total, low, high = weights[0] * v, v, v
        for k in range(1, NODES):
            v = values[k * Q + 8 * t : k * Q + 8 * t + 8]
            total = total + weights[k] * v
            low = jnp.minimum(low, v)
            high = jnp.maximum(high, v)
        clipped.append(jnp.minimum(jnp.maximum(total, low), high))
        highest.append(high)
        lowest.append(low)
    mass8 = jnp.broadcast_to(mass, (8, n))
    mh = mass8.astype(BF16).astype(F32)
    mm = mass8 - mh
    mine = level8 == sub8
    by_level = jnp.concatenate([jnp.where(mine, mh, 0.0), jnp.where(mine, mm, 0.0)], axis=0).astype(BF16)
    ch, cm = split2(jnp.concatenate(clipped, axis=0))
    sums = dot_nt(jnp.concatenate([ch, cm], axis=0), by_level)
    mmh = mm.astype(BF16).astype(F32)
    mass3 = jnp.where(sub8 == 0, mh, jnp.where(sub8 == 1, mmh, jnp.where(sub8 == 2, mm - mmh, 0.0)))
    hist = dot_nt(jnp.concatenate([mass3, mass3 * 0.0], axis=0).astype(BF16), hot)
    return clipped, highest, lowest, sums, hist, level8


def spread_terms(clipped, highest, lowest):
    margin = 0.01 + 0.05 * (highest - lowest)
    return highest + margin - clipped, clipped - lowest + margin


def fold(x):
    total = x[:, :LEVELS]
    for e in range(1, ELEMS):
        total = total + x[:, e * LEVELS : (e + 1) * LEVELS]
    return total


def level_sums(sums, hist, low_table, high_table):
    s = sums[:Q] + sums[Q:]
    clip = s[:, :LEVELS] + s[:, LEVELS:]
    mass = hist[0:1] + hist[1:2] + hist[2:3]

    s_low = fold(low_table * mass)
    s_high = fold(high_table * mass)
    margin = 0.01 * fold(jnp.broadcast_to(mass, (Q, mass.shape[1]))) + 0.05 * (s_high - s_low)
    return clip, s_high + margin - clip, clip - s_low + margin


def home_kernel(tracer_ref, old_ref, vals_ref, away_ref, table_ref, bt_ref, part_ref, hot_ref, peer_ref, c_ref, up_ref, down_ref, scratch, turns):
    rows = ELEMS * LEVELS
    node = iota((NODES, COLS), 0)
    column = iota((NODES, COLS), 1)
    wide = jnp.concatenate([jnp.where(column % NODES == node, jnp.broadcast_to(old_ref[e : e + 1, :], (NODES, COLS)), 0.0) for e in range(ELEMS)], axis=1)
    source_of = iota((ELEMS * COLS, rows), 0)
    gather = jnp.where(source_of // NODES == iota((ELEMS * COLS, rows), 1), 1.0, 0.0).astype(BF16)
    old = sum(dot(part, gather) for part in split3(wide))
    natural = tracer_ref[...].reshape(rows, NODES * Q)
    flat = [natural[:, 128 * j : 128 * (j + 1)].T for j in range(NODES * Q // 128)]
    for j, piece in enumerate(flat):
        table_ref[128 * j : 128 * (j + 1), :] = jnp.concatenate(split3(piece), axis=1)
    flat = jnp.concatenate(flat, axis=0)
    source = low = high = None
    for k in range(NODES):
        v = flat[k * Q : (k + 1) * Q]
        term = v * old[k : k + 1, :]
        source = term if source is None else source + term
        low = v if low is None else jnp.minimum(low, v)
        high = v if high is None else jnp.maximum(high, v)
    bt_ref[:Q] = low
    bt_ref[Q:] = high
    consts = node_constants(2 * COLS)
    table = table_ref[...]
    sums, hist = None, None
    for e in range(0, ELEMS, 2):
        args = [jnp.concatenate([vals_ref[v * ELEMS + e : v * ELEMS + e + 1], vals_ref[v * ELEMS + e + 1 : v * ELEMS + e + 2]], axis=1) for v in range(4)]
        clipped, highest, lowest, s, h, _ = evaluate(*args, table, consts)
        sums = s if sums is None else sums + s
        hist = h if hist is None else hist + h
        terms = [spread_terms(clipped[i], highest[i], lowest[i]) for i in range(Q // 8)]
        terms = (clipped, [t[0] for t in terms], [t[1] for t in terms])
        for j in range(2):
            stays = jnp.broadcast_to(away_ref[e + j : e + j + 1, :], (Q, COLS)) < 0
            for x, (term, ref) in enumerate(zip(terms, (c_ref, up_ref, down_ref))):
                v = jnp.concatenate([t[:, j * COLS : (j + 1) * COLS] for t in term], axis=0)
                v = jnp.concatenate([jnp.where(stays, v, 0.0), jnp.zeros((COLS - Q, COLS), F32)], axis=0)
                turns[x, e + j] = v.T
                for k in range(NODES):
                    at = (e + j) * COLS + LEVELS * k
                    ref[at : at + LEVELS, :] = turns[x, e + j, pl.ds(k, LEVELS, stride=NODES), :]
    clip, up, down = level_sums(sums, hist, low, high)
    pad = jnp.zeros((Q, COLS - 3 * LEVELS), F32)
    part_ref[...] = jnp.concatenate([fold(source) - clip, up, down, pad], axis=1)
    away = away_ref[...]
    hots, inside, whole = ranks(away)
    total = whole[0]
    for e in range(1, ELEMS):
        total = total + whole[e]
    device = iota((DEVS, COLS), 0)
    present = jnp.where(total > 0.0, 1.0, 0.0)
    earlier = jnp.where(iota((DEVS, COLS), 1) < device, 1.0, 0.0).astype(BF16)
    peer = dot(earlier, present.astype(BF16))
    ids = [jnp.sum(jnp.where(peer == float(p), present, 0.0) * device.astype(F32), axis=0, keepdims=True) for p in range(PEERS)]
    named = jnp.sum(present, axis=0, keepdims=True)
    ids = [ids[0]] + [jnp.where(named > float(p), ids[p], ids[0]) for p in range(1, PEERS)]
    peer_ref[...] = jnp.concatenate(ids + [named] * (8 - PEERS), axis=0).astype(I32)
    place = jnp.where(away < 0, -1.0, jnp.concatenate(spots(hots, inside, whole, peer * float(SLOTS)), axis=0))
    scratch[...] = jnp.concatenate([place, jnp.full((COLS - ELEMS, COLS), -1.0, F32)], axis=0).T
    turned = jnp.concatenate([scratch[pl.ds(k, LEVELS, stride=NODES), :] for k in range(NODES)], axis=0)
    lane = iota((COLS, SLOTS * 8), 1).astype(F32)
    for e in range(ELEMS):
        col = jnp.broadcast_to(turned[:, e : e + 1], (COLS, SLOTS * 8))
        hot_ref[e * COLS : (e + 1) * COLS, :] = jnp.where(col == lane, 1.0, 0.0).astype(BF16)


def serve_kernel(me_ref, req_ref, table_ref, part_ref, bt_ref, keep_ref, give_ref, ids_ref, level_ref, c_ref, up_ref, down_ref, dense, tiles):
    req = req_ref[...]
    sub = iota((DEVS, DEVS), 0)
    lane = iota((DEVS, DEVS), 1)
    high, mid = split2(req)
    first = jnp.where(iota((16, DEVS), 1) == 0, 1.0, 0.0).astype(BF16)
    asks = jnp.where(dot_nt(first, high) > 0.0, 1.0, 0.0)
    counter = jnp.concatenate([jnp.where(sub < lane, 1.0, 0.0).astype(BF16), jnp.ones((DEVS, DEVS), BF16)], axis=1)
    place = dot(asks.astype(BF16), counter)
    counted = place[:8, DEVS:].astype(I32)
    place = place[:, :DEVS]
    count = counted[0, 0]
    pick = jnp.where(jnp.broadcast_to(place[0:1], (DEVS, DEVS)) == sub.astype(F32), jnp.broadcast_to(asks[0:1], (DEVS, DEVS)), 0.0).astype(BF16)
    dense[...] = dot(jnp.concatenate([pick, pick], axis=1), jnp.concatenate([high, mid], axis=0))
    ids = dot_nt(iota((16, DEVS), 1).astype(F32).astype(BF16), pick)[:8].astype(I32)
    ids = jnp.where(iota((8, DEVS), 1) < counted, ids, me_ref[0])
    ids_ref[...] = jnp.where(iota((8, DEVS), 0) == 0, ids, counted)
    groups = [dense[pl.ds(i, DEVS // 4, stride=4), :] for i in range(4)]
    block = iota((DEVS // 4, DEVS), 1) // SLOTS
    for v in range(4):
        tile = None
        for i in range(4):
            shift = (i - v) * SLOTS % DEVS
            moved = pltpu.roll(groups[i], shift, 1) if shift else groups[i]
            tile = moved if tile is None else jnp.where(block == i, moved, tile)
        tiles[v] = tile
    consts = node_constants(2 * DEVS)

    def step(u, carry):
        args = [jnp.concatenate([tiles[v, pl.ds(2 * u, 1), :], tiles[v, pl.ds(2 * u + 1, 1), :]], axis=1) for v in range(4)]
        clipped, highest, lowest, s, h, level8 = evaluate(*args, table_ref[...], consts)
        for j in range(2):
            level_ref[pl.ds(pl.multiple_of(16 * u + 8 * j, 8), 8), :] = level8[:, j * DEVS : (j + 1) * DEVS]
        for i in range(Q // 8):
            up, down = spread_terms(clipped[i], highest[i], lowest[i])
            for j in range(2):
                at = pl.ds(pl.multiple_of(2 * Q * u + j * Q + 8 * i, 8), 8)
                c_ref[at, :] = clipped[i][:, j * DEVS : (j + 1) * DEVS]
                up_ref[at, :] = up[:, j * DEVS : (j + 1) * DEVS]
                down_ref[at, :] = down[:, j * DEVS : (j + 1) * DEVS]
        return carry[0] + s, carry[1] + h

    start = (jnp.zeros((2 * Q, 2 * LEVELS), F32), jnp.zeros((16, ELEMS * LEVELS), F32))
    start = step(1, step(0, start))
    sums, hist = lax.fori_loop(2, (count + 7) // 8, step, start)
    clip, up, down = level_sums(sums, hist, bt_ref[:Q, :], bt_ref[Q:, :])
    part = jnp.concatenate([-clip, up, down], axis=1) + part_ref[:, : 3 * LEVELS]
    packed = [part[8 * i : 8 * i + 8] for i in range(Q // 8)]
    packed.append(jnp.zeros((8, COLS - 3 * LEVELS * (Q // 8)), F32))
    packed = jnp.concatenate(packed, axis=1)
    upper = jnp.full((4, COLS), me_ref[0], I32) >= DEVS // 2
    keep_ref[...] = jnp.where(upper, packed[4:], packed[:4])
    give_ref[...] = jnp.where(upper, packed[:4], packed[4:])


def spread_kernel(keep_ref, got_ref, sums_ref):
    half = keep_ref[...] + got_ref[...]
    both = jnp.concatenate([half, half], axis=0)
    for d in range(DEVS // 2):
        sums_ref[8 * d : 8 * d + 8, :] = both


def finish_kernel(ids_ref, tot_ref, level_ref, c_ref, up_ref, down_ref, hc_ref, hu_ref, hd_ref, ans_ref, home_ref, later, sem):
    halves = []
    for core in range(2):
        at = core * 4 * (DEVS // 2)
        total = tot_ref[at : at + 8, :]
        for d in range(1, DEVS // 4):
            total = total + tot_ref[at + 8 * d : at + 8 * d + 8, :]
        halves.append(total[:4] + total[4:])
    total = jnp.concatenate(halves, axis=0)
    up_total = pltpu.roll(total, COLS - LEVELS, 1)
    down_total = pltpu.roll(total, COLS - 2 * LEVELS, 1)
    lanes = iota((8, COLS), 1)
    real = (lanes < 3 * LEVELS * (Q // 8)) & (lanes % (3 * LEVELS) < LEVELS)
    rise = jnp.where(real, jnp.maximum(total, 0.0) / up_total, 0.0)
    fall = jnp.where(real, jnp.minimum(total, 0.0) / down_total, 0.0)
    coef = [x[:, 24 * i : 24 * i + LEVELS] for x in (rise, fall) for i in range(Q // 8)]
    coef = jnp.concatenate(coef, axis=0)
    square = jnp.concatenate([coef, jnp.zeros((2 * Q, 128 - LEVELS), F32)], axis=1)
    turned = jnp.concatenate([square, jnp.zeros((128 - 2 * Q, 128), F32)], axis=0).T[:LEVELS]
    coef = jnp.concatenate(split3(coef), axis=1)

    def by_level(level8):
        hot = jnp.where(level8 == iota((8, 128), 0), 1.0, 0.0)
        c = dot(coef, jnp.concatenate([hot] * 3, axis=0).astype(BF16))
        return c[:Q], c[Q:]

    block = iota((CHUNK, DEVS), 1) // SLOTS

    first = ids_ref[...]

    def step(t, id_of):
        r, f = by_level(level_ref[pl.ds(pl.multiple_of(8 * t, 8), 8), :])
        at = pl.ds(pl.multiple_of(Q * t, 8), Q)
        out = c_ref[at, :] + r * up_ref[at, :] + f * down_ref[at, :]
        parts = [out[CHUNK * b : CHUNK * (b + 1)] for b in range(4)]
        for i in range(4):
            chunk = None
            for b in range(4):
                shift = (b - i) * SLOTS % DEVS
                moved = pltpu.roll(parts[b], shift, 1) if shift else parts[b]
                chunk = moved if chunk is None else jnp.where(block == b, moved, chunk)
            ans_ref[pl.ds(id_of(4 * t + i) * CHUNK, CHUNK), :] = chunk

    for t in range(3):
        step(t, lambda i: first[0, i])
    count = first[1, 0]

    @pl.when(count > 12)
    def _():
        copy = pltpu.make_async_copy(ids_ref, later, sem)
        copy.start()
        copy.wait()

        def more(t, carry):
            step(t, lambda i: later[0, i])
            return carry

        lax.fori_loop(3, (count + 3) // 4, more, 0)
    rises = jnp.concatenate([turned] * NODES, axis=0)
    falls = jnp.concatenate([pltpu.roll(turned, 128 - Q, 1)] * NODES, axis=0)
    for e in range(ELEMS):
        at = slice(e * COLS, (e + 1) * COLS)
        home_ref[at, :] = hc_ref[at, :] + rises * hu_ref[at, :] + falls * hd_ref[at, :]


def join_kernel(peer_ref, ans_ref, hot_ref, home_ref, out_hbm, out_ref, sem):
    block = iota((CHUNK, 128), 1) // SLOTS
    peers = peer_ref[...]
    chunks = [ans_ref[pl.ds(peers[p, 0] * CHUNK, CHUNK), :] for p in range(PEERS)]
    table = []
    for b in range(4):

        def moved(p):
            shift = (p - b) * SLOTS % 128
            return pltpu.roll(chunks[p], shift, 1) if shift else chunks[p]

        near = moved(0)
        for p in range(1, 4):
            near = jnp.where(block == p, moved(p), near)
        table.append(jnp.concatenate([near, jnp.where(block == 0, moved(4), 0.0)], axis=1))
    high, mid = split2(jnp.concatenate(table, axis=0))
    for e in range(ELEMS):
        hot = hot_ref[e * COLS : (e + 1) * COLS, :]
        at = slice(e * COLS, (e + 1) * COLS)
        v = dot_nt(hot, high) + dot_nt(hot, mid) + home_ref[at, :Q]
        out_ref[e] = jnp.concatenate([v[8 * k : 8 * k + 8] for k in range(NODES)], axis=1)
        pltpu.make_async_copy(out_ref.at[e], out_hbm.at[e], sem.at[e]).start()
    for e in range(ELEMS):
        pltpu.make_async_copy(out_ref.at[e], out_hbm.at[e], sem.at[e]).wait()


def body(tracer, old_mass, new_mass, dep_owner, dep_local, dep_coord):
    me = lax.axis_index(GROUP).astype(I32).reshape(1)
    owner = dep_owner.reshape(ELEMS, COLS)
    smem, vmem, hbm = (pl.BlockSpec(memory_space=m) for m in (pltpu.SMEM, pltpu.VMEM, pltpu.HBM))

    def near(*arrays):
        return [pltpu.with_memory_space_constraint(x, pltpu.VMEM) for x in arrays]

    def call(kernel, name, outs, in_specs, scratch, args):
        return pl.pallas_call(
            kernel,
            out_shape=tuple(pltpu.VMEM(shape, dtype) for shape, dtype in outs),
            in_specs=in_specs,
            out_specs=(vmem,) * len(outs),
            scratch_shapes=scratch,
            compiler_params=pltpu.CompilerParams(vmem_limit_bytes=20 << 20),
            name=name,
        )(*args)

    def exchange(x, chunk):
        y = lax.all_to_all(x.reshape((DEVS,) + chunk), GROUP, 0, 0, tiled=True)
        return y.reshape(x.shape)

    req, away, vals, old, near_tracer = call(
        pack_kernel,
        "pack",
        (
            ((DEVS, COLS), F32),
            ((ELEMS, COLS), I32),
            ((4 * ELEMS, COLS), F32),
            ((ELEMS, COLS), F32),
            (tracer.shape, F32),
        ),
        [smem] + [hbm] * 6,
        [
            pltpu.VMEM((ELEMS, COLS), I32),
            pltpu.VMEM((ELEMS, COLS), I32),
            pltpu.VMEM((2, ELEMS, COLS), F32),
            pltpu.VMEM((ELEMS, COLS), F32),
            pltpu.SemaphoreType.DMA((6,)),
        ],
        [me] + [pltpu.with_memory_space_constraint(x, pltpu.HBM) for x in (owner, dep_local, dep_coord, new_mass, old_mass, tracer)],
    )
    asked = exchange(req, (1, COLS))
    table, bt, part, hot, peer, hc, hu, hd = call(
        home_kernel,
        "home",
        (
            ((NODES * Q, 3 * ELEMS * LEVELS), BF16),
            ((2 * Q, ELEMS * LEVELS), F32),
            ((Q, COLS), F32),
            ((ELEMS * COLS, SLOTS * 8), BF16),
            ((8, COLS), I32),
        )
        + (((ELEMS * COLS, 128), F32),) * 3,
        [vmem] * 4,
        [pltpu.VMEM((COLS, COLS), F32), pltpu.VMEM((3, ELEMS, COLS, 128), F32)],
        near(near_tracer, old, vals, away),
    )
    keep, give, ids, level, c, up, down = call(
        serve_kernel,
        "serve",
        (((4, COLS), F32), ((4, COLS), F32), ((8, DEVS), I32), ((2 * DEVS, DEVS), I32)) + (((SLOTS * Q, DEVS), F32),) * 3,
        [smem] + [vmem] * 4,
        [pltpu.VMEM((DEVS, DEVS), F32), pltpu.VMEM((4, DEVS // 4, DEVS), F32)],
        [me] + near(asked, table, part, bt),
    )
    given = lax.ppermute(give, "core", [(0, 1), (1, 0)])
    (sums,) = call(spread_kernel, "spread", (((4 * DEVS, COLS), F32),), [vmem] * 2, [], near(keep, given))
    totals = exchange(sums, (4, COLS))
    ans, home = call(
        finish_kernel,
        "finish",
        (((DEVS * CHUNK, 128), F32), ((ELEMS * COLS, 128), F32)),
        [vmem] * 9,
        [pltpu.SMEM((8, DEVS), I32), pltpu.SemaphoreType.DMA],
        near(ids, totals, level, c, up, down, hc, hu, hd),
    )
    got = exchange(ans, (1, SLOTS * Q))
    return pl.pallas_call(
        join_kernel,
        out_shape=jax.ShapeDtypeStruct((ELEMS, LEVELS, NODES * Q), F32),
        in_specs=[vmem] * 4,
        out_specs=hbm,
        scratch_shapes=[pltpu.VMEM((ELEMS, LEVELS, NODES * Q), F32), pltpu.SemaphoreType.DMA((ELEMS,))],
        compiler_params=pltpu.CompilerParams(vmem_limit_bytes=20 << 20),
        name="join",
    )(*near(peer, got, hot, home))


def solution(mesh):
    torus = Mesh(mesh.devices.reshape(4, 4, 4, 2), AXES)
    placed = (
        P(AXES, None, None),
        P(AXES, None),
        P(AXES, None),
        P(AXES, None, None),
        P(AXES, None),
        P(None, AXES, None),
    )
    return jax.shard_map(body, mesh=torus, in_specs=placed, out_specs=P(AXES, None, None), check_vma=False)
```

```python
import jax
import jax.numpy as jnp
from jax import lax
from jax.experimental import pallas as pl
from jax.experimental.pallas import tpu as pltpu
from jax.sharding import Mesh
from jax.sharding import PartitionSpec as P

AXES = ("x", "y", "z", "core")
GROUP = ("core", "z", "y", "x")
GLL = (-1.0, -0.4472135954999579, 0.4472135954999579, 1.0)
DEVS = 128
ELEMS = 8
LEVELS = 8
NODES = 16
Q = 40
SLOTS = 32
PEERS = 5
COLS = LEVELS * NODES
CHUNK = SLOTS * Q // 128
F32, BF16, I32 = jnp.float32, jnp.bfloat16, jnp.int32
NT = (((1,), (1,)), ((), ()))


def iota(shape, dim):
    return lax.broadcasted_iota(I32, shape, dim)


def in_group(device):
    core, z, y, x = device % 2, device // 2 % 4, device // 8 % 4, device // 32
    return core * 64 + z * 16 + y * 4 + x


def dot(a, b):
    return jnp.dot(a, b, preferred_element_type=F32)


def dot_nt(a, b):
    return lax.dot_general(a, b, NT, preferred_element_type=F32)


def split2(x):
    high = x.astype(BF16)
    return high, (x - high.astype(F32)).astype(BF16)


def split3(x):
    high = x.astype(BF16)
    rest = x - high.astype(F32)
    mid = rest.astype(BF16)
    return high, mid, (rest - mid.astype(F32)).astype(BF16)


def ranks(owner):
    sub = iota((DEVS, COLS), 0)
    before = jnp.where(sub < iota((DEVS, COLS), 1), 1.0, 0.0).astype(BF16)
    counter = jnp.concatenate([before, jnp.ones((COLS, COLS), BF16)], axis=1)
    hots = [jnp.where(jnp.broadcast_to(owner[e : e + 1], (DEVS, COLS)) == sub, 1.0, 0.0) for e in range(ELEMS)]
    counts = dot(jnp.concatenate(hots, axis=0).astype(BF16), counter)
    parts = [counts[e * DEVS : (e + 1) * DEVS] for e in range(ELEMS)]
    return hots, [p[:, :COLS] for p in parts], [p[:, COLS:] for p in parts]


def spots(hots, inside, whole, base):
    rows = []
    for e in range(ELEMS):
        rows.append(jnp.sum(hots[e] * (inside[e] + base), axis=0, keepdims=True))
        base = base + whole[e]
    return rows


def pack_kernel(me_ref, owner_hbm, local_hbm, coord_hbm, mass_hbm, old_hbm, tracer_hbm, req_ref, away_ref, vals_ref, old_ref, tracer_ref, owner_ref, local_ref, coord_ref, mass_ref, sem):
    pairs = (
        (owner_hbm, owner_ref),
        (local_hbm, local_ref),
        (coord_hbm, coord_ref),
        (mass_hbm, mass_ref),
        (old_hbm, old_ref),
        (tracer_hbm, tracer_ref),
    )
    copies = [pltpu.make_async_copy(src, dst, sem.at[i]) for i, (src, dst) in enumerate(pairs)]
    for copy in copies:
        copy.start()
    me = me_ref[0]
    for copy in copies[:4]:
        copy.wait()
    owner = in_group(owner_ref[...])
    owner = jnp.where(owner == me, -1, owner)
    away_ref[...] = owner
    level = iota((ELEMS, COLS), 1) // NODES
    row = (local_ref[...] * LEVELS + (level + 1)).astype(F32)
    mass = mass_ref[...]
    vals_ref[:ELEMS] = row
    vals_ref[ELEMS : 2 * ELEMS] = coord_ref[0]
    vals_ref[2 * ELEMS : 3 * ELEMS] = coord_ref[1]
    vals_ref[3 * ELEMS :] = jnp.where(owner < 0, mass, 0.0)
    values = (row, coord_ref[0], coord_ref[1], mass)
    hots, inside, whole = ranks(owner)
    slot = (iota((DEVS, COLS), 0) % SLOTS).astype(F32)
    wide = []
    for e, spot in enumerate(spots(hots, inside, whole, jnp.zeros((DEVS, COLS), F32))):
        value = jnp.concatenate([jnp.broadcast_to(v[e : e + 1], (SLOTS, COLS)) for v in values], axis=0)
        wide.append(jnp.where(jnp.broadcast_to(spot, (DEVS, COLS)) == slot, value, 0.0))
    hot = jnp.concatenate(hots, axis=1).astype(BF16)
    high, mid = split2(jnp.concatenate(wide, axis=1))
    req_ref[...] = dot_nt(hot, high) + dot_nt(hot, mid)
    for copy in copies[4:]:
        copy.wait()


def node_constants(n):
    def one(index):
        p0 = jnp.where(index > 0, GLL[0], GLL[1])
        p1 = jnp.where(index > 1, GLL[1], GLL[2])
        p2 = jnp.where(index > 2, GLL[2], GLL[3])
        scale = []
        for i in range(4):
            prod = 1.0
            for j in range(4):
                if j != i:
                    prod *= GLL[i] - GLL[j]
            scale.append(1.0 / prod)
        c = jnp.where(index == 0, scale[0], jnp.where(index == 1, scale[1], jnp.where(index == 2, scale[2], scale[3])))
        return p0, p1, p2, c

    k = iota((NODES, n), 0)
    return one(k // 4), one(k % 4)


def lagrange(x, consts):
    p0, p1, p2, c = consts
    return ((x - p0) * (x - p1)) * ((x - p2) * c)


def evaluate(row, a, b, mass, table, consts):
    n = row.shape[1]
    index = jnp.maximum(row.astype(I32) - 1, 0)
    index8 = jnp.broadcast_to(index, (8, n))
    level8 = index8 % LEVELS
    sub8 = iota((8, n), 0)
    hot = jnp.concatenate([jnp.where(index8 == sub8 + 8 * e, 1.0, 0.0) for e in range(ELEMS)], axis=0).astype(BF16)
    values = dot(table, jnp.concatenate([hot, hot, hot], axis=0))
    w = lagrange(jnp.broadcast_to(a, (NODES, n)), consts[0]) * lagrange(jnp.broadcast_to(b, (NODES, n)), consts[1])
    weights = [jnp.broadcast_to(w[k : k + 1], (8, n)) for k in range(NODES)]
    clipped, highest, lowest = [], [], []
    for t in range(Q // 8):
        v = values[8 * t : 8 * t + 8]
        total, low, high = weights[0] * v, v, v
        for k in range(1, NODES):
            v = values[k * Q + 8 * t : k * Q + 8 * t + 8]
            total = total + weights[k] * v
            low = jnp.minimum(low, v)
            high = jnp.maximum(high, v)
        clipped.append(jnp.minimum(jnp.maximum(total, low), high))
        highest.append(high)
        lowest.append(low)
    mass8 = jnp.broadcast_to(mass, (8, n))
    mh = mass8.astype(BF16).astype(F32)
    mm = mass8 - mh
    mine = level8 == sub8
    by_level = jnp.concatenate([jnp.where(mine, mh, 0.0), jnp.where(mine, mm, 0.0)], axis=0).astype(BF16)
    ch, cm = split2(jnp.concatenate(clipped, axis=0))
    sums = dot_nt(jnp.concatenate([ch, cm], axis=0), by_level)
    mmh = mm.astype(BF16).astype(F32)
    mass3 = jnp.where(sub8 == 0, mh, jnp.where(sub8 == 1, mmh, jnp.where(sub8 == 2, mm - mmh, 0.0)))
    hist = dot_nt(jnp.concatenate([mass3, mass3 * 0.0], axis=0).astype(BF16), hot)
    return clipped, highest, lowest, sums, hist, level8


def spread_terms(clipped, highest, lowest):
    margin = 0.01 + 0.05 * (highest - lowest)
    return highest + margin - clipped, clipped - lowest + margin


def fold(x):
    total = x[:, :LEVELS]
    for e in range(1, ELEMS):
        total = total + x[:, e * LEVELS : (e + 1) * LEVELS]
    return total


def level_sums(sums, hist, low_table, high_table):
    s = sums[:Q] + sums[Q:]
    clip = s[:, :LEVELS] + s[:, LEVELS:]
    mass = hist[0:1] + hist[1:2] + hist[2:3]

    s_low = fold(low_table * mass)
    s_high = fold(high_table * mass)
    margin = 0.01 * fold(jnp.broadcast_to(mass, (Q, mass.shape[1]))) + 0.05 * (s_high - s_low)
    return clip, s_high + margin - clip, clip - s_low + margin


def home_kernel(tracer_ref, old_ref, vals_ref, away_ref, table_ref, bt_ref, part_ref, hot_ref, peer_ref, c_ref, up_ref, down_ref, scratch, turns):
    rows = ELEMS * LEVELS
    node = iota((NODES, COLS), 0)
    column = iota((NODES, COLS), 1)
    wide = jnp.concatenate([jnp.where(column % NODES == node, jnp.broadcast_to(old_ref[e : e + 1, :], (NODES, COLS)), 0.0) for e in range(ELEMS)], axis=1)
    source_of = iota((ELEMS * COLS, rows), 0)
    gather = jnp.where(source_of // NODES == iota((ELEMS * COLS, rows), 1), 1.0, 0.0).astype(BF16)
    old = sum(dot(part, gather) for part in split3(wide))
    natural = tracer_ref[...].reshape(rows, NODES * Q)
    flat = [natural[:, 128 * j : 128 * (j + 1)].T for j in range(NODES * Q // 128)]
    for j, piece in enumerate(flat):
        table_ref[128 * j : 128 * (j + 1), :] = jnp.concatenate(split3(piece), axis=1)
    flat = jnp.concatenate(flat, axis=0)
    source = low = high = None
    for k in range(NODES):
        v = flat[k * Q : (k + 1) * Q]
        term = v * old[k : k + 1, :]
        source = term if source is None else source + term
        low = v if low is None else jnp.minimum(low, v)
        high = v if high is None else jnp.maximum(high, v)
    bt_ref[:Q] = low
    bt_ref[Q:] = high
    consts = node_constants(2 * COLS)
    table = table_ref[...]
    sums, hist = None, None
    for e in range(0, ELEMS, 2):
        args = [jnp.concatenate([vals_ref[v * ELEMS + e : v * ELEMS + e + 1], vals_ref[v * ELEMS + e + 1 : v * ELEMS + e + 2]], axis=1) for v in range(4)]
        clipped, highest, lowest, s, h, _ = evaluate(*args, table, consts)
        sums = s if sums is None else sums + s
        hist = h if hist is None else hist + h
        terms = [spread_terms(clipped[i], highest[i], lowest[i]) for i in range(Q // 8)]
        terms = (clipped, [t[0] for t in terms], [t[1] for t in terms])
        for j in range(2):
            stays = jnp.broadcast_to(away_ref[e + j : e + j + 1, :], (Q, COLS)) < 0
            for x, (term, ref) in enumerate(zip(terms, (c_ref, up_ref, down_ref))):
                v = jnp.concatenate([t[:, j * COLS : (j + 1) * COLS] for t in term], axis=0)
                v = jnp.concatenate([jnp.where(stays, v, 0.0), jnp.zeros((COLS - Q, COLS), F32)], axis=0)
                turns[x, e + j] = v.T
                for k in range(NODES):
                    at = (e + j) * COLS + LEVELS * k
                    ref[at : at + LEVELS, :] = turns[x, e + j, pl.ds(k, LEVELS, stride=NODES), :]
    clip, up, down = level_sums(sums, hist, low, high)
    pad = jnp.zeros((Q, COLS - 3 * LEVELS), F32)
    part_ref[...] = jnp.concatenate([fold(source) - clip, up, down, pad], axis=1)
    away = away_ref[...]
    hots, inside, whole = ranks(away)
    total = whole[0]
    for e in range(1, ELEMS):
        total = total + whole[e]
    device = iota((DEVS, COLS), 0)
    present = jnp.where(total > 0.0, 1.0, 0.0)
    earlier = jnp.where(iota((DEVS, COLS), 1) < device, 1.0, 0.0).astype(BF16)
    peer = dot(earlier, present.astype(BF16))
    ids = [jnp.sum(jnp.where(peer == float(p), present, 0.0) * device.astype(F32), axis=0, keepdims=True) for p in range(PEERS)]
    named = jnp.sum(present, axis=0, keepdims=True)
    ids = [ids[0]] + [jnp.where(named > float(p), ids[p], ids[0]) for p in range(1, PEERS)]
    peer_ref[...] = jnp.concatenate(ids + [named] * (8 - PEERS), axis=0).astype(I32)
    place = jnp.where(away < 0, -1.0, jnp.concatenate(spots(hots, inside, whole, peer * float(SLOTS)), axis=0))
    scratch[...] = jnp.concatenate([place, jnp.full((COLS - ELEMS, COLS), -1.0, F32)], axis=0).T
    turned = jnp.concatenate([scratch[pl.ds(k, LEVELS, stride=NODES), :] for k in range(NODES)], axis=0)
    lane = iota((COLS, SLOTS * 8), 1).astype(F32)
    for e in range(ELEMS):
        col = jnp.broadcast_to(turned[:, e : e + 1], (COLS, SLOTS * 8))
        hot_ref[e * COLS : (e + 1) * COLS, :] = jnp.where(col == lane, 1.0, 0.0).astype(BF16)


def serve_kernel(me_ref, req_ref, table_ref, part_ref, bt_ref, keep_ref, give_ref, ids_ref, level_ref, c_ref, up_ref, down_ref, dense, tiles):
    req = req_ref[...]
    sub = iota((DEVS, DEVS), 0)
    lane = iota((DEVS, DEVS), 1)
    high, mid = split2(req)
    first = jnp.where(iota((16, DEVS), 1) == 0, 1.0, 0.0).astype(BF16)
    asks = jnp.where(dot_nt(first, high) > 0.0, 1.0, 0.0)
    counter = jnp.concatenate([jnp.where(sub < lane, 1.0, 0.0).astype(BF16), jnp.ones((DEVS, DEVS), BF16)], axis=1)
    place = dot(asks.astype(BF16), counter)
    counted = place[:8, DEVS:].astype(I32)
    place = place[:, :DEVS]
    count = counted[0, 0]
    pick = jnp.where(jnp.broadcast_to(place[0:1], (DEVS, DEVS)) == sub.astype(F32), jnp.broadcast_to(asks[0:1], (DEVS, DEVS)), 0.0).astype(BF16)
    dense[...] = dot(jnp.concatenate([pick, pick], axis=1), jnp.concatenate([high, mid], axis=0))
    ids = dot_nt(iota((16, DEVS), 1).astype(F32).astype(BF16), pick)[:8].astype(I32)
    ids = jnp.where(iota((8, DEVS), 1) < counted, ids, me_ref[0])
    ids_ref[...] = jnp.where(iota((8, DEVS), 0) == 0, ids, counted)
    groups = [dense[pl.ds(i, DEVS // 4, stride=4), :] for i in range(4)]
    block = iota((DEVS // 4, DEVS), 1) // SLOTS
    for v in range(4):
        tile = None
        for i in range(4):
            shift = (i - v) * SLOTS % DEVS
            moved = pltpu.roll(groups[i], shift, 1) if shift else groups[i]
            tile = moved if tile is None else jnp.where(block == i, moved, tile)
        tiles[v] = tile
    consts = node_constants(2 * DEVS)

    def step(u, carry):
        args = [jnp.concatenate([tiles[v, pl.ds(2 * u, 1), :], tiles[v, pl.ds(2 * u + 1, 1), :]], axis=1) for v in range(4)]
        clipped, highest, lowest, s, h, level8 = evaluate(*args, table_ref[...], consts)
        for j in range(2):
            level_ref[pl.ds(pl.multiple_of(16 * u + 8 * j, 8), 8), :] = level8[:, j * DEVS : (j + 1) * DEVS]
        for i in range(Q // 8):
            up, down = spread_terms(clipped[i], highest[i], lowest[i])
            for j in range(2):
                at = pl.ds(pl.multiple_of(2 * Q * u + j * Q + 8 * i, 8), 8)
                c_ref[at, :] = clipped[i][:, j * DEVS : (j + 1) * DEVS]
                up_ref[at, :] = up[:, j * DEVS : (j + 1) * DEVS]
                down_ref[at, :] = down[:, j * DEVS : (j + 1) * DEVS]
        return carry[0] + s, carry[1] + h

    start = (jnp.zeros((2 * Q, 2 * LEVELS), F32), jnp.zeros((16, ELEMS * LEVELS), F32))
    start = step(1, step(0, start))
    sums, hist = lax.fori_loop(2, (count + 7) // 8, step, start)
    clip, up, down = level_sums(sums, hist, bt_ref[:Q, :], bt_ref[Q:, :])
    part = jnp.concatenate([-clip, up, down], axis=1) + part_ref[:, : 3 * LEVELS]
    packed = [part[8 * i : 8 * i + 8] for i in range(Q // 8)]
    packed.append(jnp.zeros((8, COLS - 3 * LEVELS * (Q // 8)), F32))
    packed = jnp.concatenate(packed, axis=1)
    upper = jnp.full((4, COLS), me_ref[0], I32) >= DEVS // 2
    keep_ref[...] = jnp.where(upper, packed[4:], packed[:4])
    give_ref[...] = jnp.where(upper, packed[:4], packed[4:])


def spread_kernel(keep_ref, got_ref, sums_ref):
    half = keep_ref[...] + got_ref[...]
    both = jnp.concatenate([half, half], axis=0)
    for d in range(DEVS // 2):
        sums_ref[8 * d : 8 * d + 8, :] = both


def finish_kernel(ids_ref, tot_ref, level_ref, c_ref, up_ref, down_ref, hc_ref, hu_ref, hd_ref, ans_ref, home_ref, later, sem):
    halves = []
    for core in range(2):
        at = core * 4 * (DEVS // 2)
        total = tot_ref[at : at + 8, :]
        for d in range(1, DEVS // 4):
            total = total + tot_ref[at + 8 * d : at + 8 * d + 8, :]
        halves.append(total[:4] + total[4:])
    total = jnp.concatenate(halves, axis=0)
    up_total = pltpu.roll(total, COLS - LEVELS, 1)
    down_total = pltpu.roll(total, COLS - 2 * LEVELS, 1)
    lanes = iota((8, COLS), 1)
    real = (lanes < 3 * LEVELS * (Q // 8)) & (lanes % (3 * LEVELS) < LEVELS)
    rise = jnp.where(real, jnp.maximum(total, 0.0) / up_total, 0.0)
    fall = jnp.where(real, jnp.minimum(total, 0.0) / down_total, 0.0)
    coef = [x[:, 24 * i : 24 * i + LEVELS] for x in (rise, fall) for i in range(Q // 8)]
    coef = jnp.concatenate(coef, axis=0)
    square = jnp.concatenate([coef, jnp.zeros((2 * Q, 128 - LEVELS), F32)], axis=1)
    turned = jnp.concatenate([square, jnp.zeros((128 - 2 * Q, 128), F32)], axis=0).T[:LEVELS]
    coef = jnp.concatenate(split3(coef), axis=1)

    def by_level(level8):
        hot = jnp.where(level8 == iota((8, 128), 0), 1.0, 0.0)
        c = dot(coef, jnp.concatenate([hot] * 3, axis=0).astype(BF16))
        return c[:Q], c[Q:]

    block = iota((CHUNK, DEVS), 1) // SLOTS

    first = ids_ref[...]

    def step(t, id_of):
        r, f = by_level(level_ref[pl.ds(pl.multiple_of(8 * t, 8), 8), :])
        at = pl.ds(pl.multiple_of(Q * t, 8), Q)
        out = c_ref[at, :] + r * up_ref[at, :] + f * down_ref[at, :]
        parts = [out[CHUNK * b : CHUNK * (b + 1)] for b in range(4)]
        for i in range(4):
            chunk = None
            for b in range(4):
                shift = (b - i) * SLOTS % DEVS
                moved = pltpu.roll(parts[b], shift, 1) if shift else parts[b]
                chunk = moved if chunk is None else jnp.where(block == b, moved, chunk)
            ans_ref[pl.ds(id_of(4 * t + i) * CHUNK, CHUNK), :] = chunk

    for t in range(3):
        step(t, lambda i: first[0, i])
    count = first[1, 0]

    @pl.when(count > 12)
    def _():
        copy = pltpu.make_async_copy(ids_ref, later, sem)
        copy.start()
        copy.wait()

        def more(t, carry):
            step(t, lambda i: later[0, i])
            return carry

        lax.fori_loop(3, (count + 3) // 4, more, 0)
    rises = jnp.concatenate([turned] * NODES, axis=0)
    falls = jnp.concatenate([pltpu.roll(turned, 128 - Q, 1)] * NODES, axis=0)
    for e in range(ELEMS):
        at = slice(e * COLS, (e + 1) * COLS)
        home_ref[at, :] = hc_ref[at, :] + rises * hu_ref[at, :] + falls * hd_ref[at, :]


def join_kernel(peer_ref, ans_ref, hot_ref, home_ref, out_hbm, out_ref, sem):
    block = iota((CHUNK, 128), 1) // SLOTS
    peers = peer_ref[...]
    chunks = [ans_ref[pl.ds(peers[p, 0] * CHUNK, CHUNK), :] for p in range(PEERS)]
    table = []
    for b in range(4):

        def moved(p):
            shift = (p - b) * SLOTS % 128
            return pltpu.roll(chunks[p], shift, 1) if shift else chunks[p]

        near = moved(0)
        for p in range(1, 4):
            near = jnp.where(block == p, moved(p), near)
        table.append(jnp.concatenate([near, jnp.where(block == 0, moved(4), 0.0)], axis=1))
    high, mid = split2(jnp.concatenate(table, axis=0))
    both = jnp.concatenate([high, mid], axis=0)
    for e in range(ELEMS):
        picked = dot_nt(hot_ref[e * COLS : (e + 1) * COLS, :], both)
        v = picked[:, :Q] + picked[:, Q:] + home_ref[e * COLS : (e + 1) * COLS, :Q]
        out_ref[e] = jnp.concatenate([v[8 * k : 8 * k + 8] for k in range(NODES)], axis=1)
        pltpu.make_async_copy(out_ref.at[e], out_hbm.at[e], sem.at[e]).start()
    for e in range(ELEMS):
        pltpu.make_async_copy(out_ref.at[e], out_hbm.at[e], sem.at[e]).wait()


def body(tracer, old_mass, new_mass, dep_owner, dep_local, dep_coord):
    me = lax.axis_index(GROUP).astype(I32).reshape(1)
    owner = dep_owner.reshape(ELEMS, COLS)
    smem, vmem, hbm = (pl.BlockSpec(memory_space=m) for m in (pltpu.SMEM, pltpu.VMEM, pltpu.HBM))

    def near(*arrays):
        return [pltpu.with_memory_space_constraint(x, pltpu.VMEM) for x in arrays]

    def call(kernel, name, outs, in_specs, scratch, args):
        return pl.pallas_call(
            kernel,
            out_shape=tuple(pltpu.VMEM(shape, dtype) for shape, dtype in outs),
            in_specs=in_specs,
            out_specs=(vmem,) * len(outs),
            scratch_shapes=scratch,
            compiler_params=pltpu.CompilerParams(vmem_limit_bytes=20 << 20),
            name=name,
        )(*args)

    def exchange(x, chunk):
        y = lax.all_to_all(x.reshape((DEVS,) + chunk), GROUP, 0, 0, tiled=True)
        return y.reshape(x.shape)

    req, away, vals, old, near_tracer = call(
        pack_kernel,
        "pack",
        (
            ((DEVS, COLS), F32),
            ((ELEMS, COLS), I32),
            ((4 * ELEMS, COLS), F32),
            ((ELEMS, COLS), F32),
            (tracer.shape, F32),
        ),
        [smem] + [hbm] * 6,
        [
            pltpu.VMEM((ELEMS, COLS), I32),
            pltpu.VMEM((ELEMS, COLS), I32),
            pltpu.VMEM((2, ELEMS, COLS), F32),
            pltpu.VMEM((ELEMS, COLS), F32),
            pltpu.SemaphoreType.DMA((6,)),
        ],
        [me] + [pltpu.with_memory_space_constraint(x, pltpu.HBM) for x in (owner, dep_local, dep_coord, new_mass, old_mass, tracer)],
    )
    asked = exchange(req, (1, COLS))
    table, bt, part, hot, peer, hc, hu, hd = call(
        home_kernel,
        "home",
        (
            ((NODES * Q, 3 * ELEMS * LEVELS), BF16),
            ((2 * Q, ELEMS * LEVELS), F32),
            ((Q, COLS), F32),
            ((ELEMS * COLS, SLOTS * 8), BF16),
            ((8, COLS), I32),
        )
        + (((ELEMS * COLS, 128), F32),) * 3,
        [vmem] * 4,
        [pltpu.VMEM((COLS, COLS), F32), pltpu.VMEM((3, ELEMS, COLS, 128), F32)],
        near(near_tracer, old, vals, away),
    )
    keep, give, ids, level, c, up, down = call(
        serve_kernel,
        "serve",
        (((4, COLS), F32), ((4, COLS), F32), ((8, DEVS), I32), ((2 * DEVS, DEVS), I32)) + (((SLOTS * Q, DEVS), F32),) * 3,
        [smem] + [vmem] * 4,
        [pltpu.VMEM((DEVS, DEVS), F32), pltpu.VMEM((4, DEVS // 4, DEVS), F32)],
        [me] + near(asked, table, part, bt),
    )
    given = lax.ppermute(give, "core", [(0, 1), (1, 0)])
    (sums,) = call(spread_kernel, "spread", (((4 * DEVS, COLS), F32),), [vmem] * 2, [], near(keep, given))
    totals = exchange(sums, (4, COLS))
    ans, home = call(
        finish_kernel,
        "finish",
        (((DEVS * CHUNK, 128), F32), ((ELEMS * COLS, 128), F32)),
        [vmem] * 9,
        [pltpu.SMEM((8, DEVS), I32), pltpu.SemaphoreType.DMA],
        near(ids, totals, level, c, up, down, hc, hu, hd),
    )
    got = exchange(ans, (1, SLOTS * Q))
    return pl.pallas_call(
        join_kernel,
        out_shape=jax.ShapeDtypeStruct((ELEMS, LEVELS, NODES * Q), F32),
        in_specs=[vmem] * 4,
        out_specs=hbm,
        scratch_shapes=[pltpu.VMEM((ELEMS, LEVELS, NODES * Q), F32), pltpu.SemaphoreType.DMA((ELEMS,))],
        compiler_params=pltpu.CompilerParams(vmem_limit_bytes=20 << 20),
        name="join",
    )(*near(peer, got, hot, home))


def solution(mesh):
    torus = Mesh(mesh.devices.reshape(4, 4, 4, 2), AXES)
    placed = (
        P(AXES, None, None),
        P(AXES, None),
        P(AXES, None),
        P(AXES, None, None),
        P(AXES, None),
        P(None, AXES, None),
    )
    return jax.shard_map(body, mesh=torus, in_specs=placed, out_specs=P(AXES, None, None), check_vma=False)
```

```python
import jax
import jax.numpy as jnp
from jax import lax
from jax.experimental import pallas as pl
from jax.experimental.pallas import tpu as pltpu
from jax.sharding import Mesh
from jax.sharding import PartitionSpec as P

AXES = ("x", "y", "z", "core")
GROUP = ("core", "z", "y", "x")
GLL = (-1.0, -0.4472135954999579, 0.4472135954999579, 1.0)
DEVS = 128
ELEMS = 8
LEVELS = 8
NODES = 16
Q = 40
SLOTS = 32
PEERS = 5
COLS = LEVELS * NODES
CHUNK = SLOTS * Q // 128
F32, BF16, I32 = jnp.float32, jnp.bfloat16, jnp.int32
NT = (((1,), (1,)), ((), ()))


def iota(shape, dim):
    return lax.broadcasted_iota(I32, shape, dim)


def in_group(device):
    core, z, y, x = device % 2, device // 2 % 4, device // 8 % 4, device // 32
    return core * 64 + z * 16 + y * 4 + x


def dot(a, b):
    return jnp.dot(a, b, preferred_element_type=F32)


def dot_nt(a, b):
    return lax.dot_general(a, b, NT, preferred_element_type=F32)


def split2(x):
    high = x.astype(BF16)
    return high, (x - high.astype(F32)).astype(BF16)


def split3(x):
    high = x.astype(BF16)
    rest = x - high.astype(F32)
    mid = rest.astype(BF16)
    return high, mid, (rest - mid.astype(F32)).astype(BF16)


def ranks(owner):
    sub = iota((DEVS, COLS), 0)
    before = jnp.where(sub < iota((DEVS, COLS), 1), 1.0, 0.0).astype(BF16)
    counter = jnp.concatenate([before, jnp.ones((COLS, COLS), BF16)], axis=1)
    hots = [jnp.where(jnp.broadcast_to(owner[e : e + 1], (DEVS, COLS)) == sub, 1.0, 0.0) for e in range(ELEMS)]
    counts = dot(jnp.concatenate(hots, axis=0).astype(BF16), counter)
    parts = [counts[e * DEVS : (e + 1) * DEVS] for e in range(ELEMS)]
    return hots, [p[:, :COLS] for p in parts], [p[:, COLS:] for p in parts]


def spots(hots, inside, whole, base):
    rows = []
    for e in range(ELEMS):
        rows.append(jnp.sum(hots[e] * (inside[e] + base), axis=0, keepdims=True))
        base = base + whole[e]
    return rows


def pack_kernel(me_ref, owner_hbm, local_hbm, coord_hbm, mass_hbm, old_hbm, tracer_hbm, req_ref, away_ref, vals_ref, old_ref, tracer_ref, owner_ref, local_ref, coord_ref, mass_ref, sem):
    pairs = (
        (owner_hbm, owner_ref),
        (local_hbm, local_ref),
        (coord_hbm, coord_ref),
        (mass_hbm, mass_ref),
        (old_hbm, old_ref),
        (tracer_hbm, tracer_ref),
    )
    copies = [pltpu.make_async_copy(src, dst, sem.at[i]) for i, (src, dst) in enumerate(pairs)]
    for copy in copies:
        copy.start()
    me = me_ref[0]
    for copy in copies[:4]:
        copy.wait()
    owner = in_group(owner_ref[...])
    owner = jnp.where(owner == me, -1, owner)
    away_ref[...] = owner
    level = iota((ELEMS, COLS), 1) // NODES
    row = (local_ref[...] * LEVELS + (level + 1)).astype(F32)
    mass = mass_ref[...]
    vals_ref[:ELEMS] = row
    vals_ref[ELEMS : 2 * ELEMS] = coord_ref[0]
    vals_ref[2 * ELEMS : 3 * ELEMS] = coord_ref[1]
    vals_ref[3 * ELEMS :] = jnp.where(owner < 0, mass, 0.0)
    values = (row, coord_ref[0], coord_ref[1], mass)
    hots, inside, whole = ranks(owner)
    slot = (iota((DEVS, COLS), 0) % SLOTS).astype(F32)
    wide = []
    for e, spot in enumerate(spots(hots, inside, whole, jnp.zeros((DEVS, COLS), F32))):
        value = jnp.concatenate([jnp.broadcast_to(v[e : e + 1], (SLOTS, COLS)) for v in values], axis=0)
        wide.append(jnp.where(jnp.broadcast_to(spot, (DEVS, COLS)) == slot, value, 0.0))
    hot = jnp.concatenate(hots, axis=1).astype(BF16)
    high, mid = split2(jnp.concatenate(wide, axis=1))
    req_ref[...] = dot_nt(hot, high) + dot_nt(hot, mid)
    for copy in copies[4:]:
        copy.wait()


def node_constants(n):
    def one(index):
        p0 = jnp.where(index > 0, GLL[0], GLL[1])
        p1 = jnp.where(index > 1, GLL[1], GLL[2])
        p2 = jnp.where(index > 2, GLL[2], GLL[3])
        scale = []
        for i in range(4):
            prod = 1.0
            for j in range(4):
                if j != i:
                    prod *= GLL[i] - GLL[j]
            scale.append(1.0 / prod)
        c = jnp.where(index == 0, scale[0], jnp.where(index == 1, scale[1], jnp.where(index == 2, scale[2], scale[3])))
        return p0, p1, p2, c

    k = iota((NODES, n), 0)
    return one(k // 4), one(k % 4)


def lagrange(x, consts):
    p0, p1, p2, c = consts
    return ((x - p0) * (x - p1)) * ((x - p2) * c)


def evaluate(row, a, b, mass, table, consts):
    n = row.shape[1]
    index = jnp.maximum(row.astype(I32) - 1, 0)
    index8 = jnp.broadcast_to(index, (8, n))
    level8 = index8 % LEVELS
    sub8 = iota((8, n), 0)
    hot = jnp.concatenate([jnp.where(index8 == sub8 + 8 * e, 1.0, 0.0) for e in range(ELEMS)], axis=0).astype(BF16)
    values = dot(table, jnp.concatenate([hot, hot, hot], axis=0))
    w = lagrange(jnp.broadcast_to(a, (NODES, n)), consts[0]) * lagrange(jnp.broadcast_to(b, (NODES, n)), consts[1])
    weights = [jnp.broadcast_to(w[k : k + 1], (8, n)) for k in range(NODES)]
    clipped, highest, lowest = [], [], []
    for t in range(Q // 8):
        v = values[8 * t : 8 * t + 8]
        total, low, high = weights[0] * v, v, v
        for k in range(1, NODES):
            v = values[k * Q + 8 * t : k * Q + 8 * t + 8]
            total = total + weights[k] * v
            low = jnp.minimum(low, v)
            high = jnp.maximum(high, v)
        clipped.append(jnp.minimum(jnp.maximum(total, low), high))
        highest.append(high)
        lowest.append(low)
    mass8 = jnp.broadcast_to(mass, (8, n))
    mh = mass8.astype(BF16).astype(F32)
    mm = mass8 - mh
    mine = level8 == sub8
    by_level = jnp.concatenate([jnp.where(mine, mh, 0.0), jnp.where(mine, mm, 0.0)], axis=0).astype(BF16)
    ch, cm = split2(jnp.concatenate(clipped, axis=0))
    sums = dot_nt(jnp.concatenate([ch, cm], axis=0), by_level)
    mmh = mm.astype(BF16).astype(F32)
    mass3 = jnp.where(sub8 == 0, mh, jnp.where(sub8 == 1, mmh, jnp.where(sub8 == 2, mm - mmh, 0.0)))
    hist = dot_nt(jnp.concatenate([mass3, mass3 * 0.0], axis=0).astype(BF16), hot)
    return clipped, highest, lowest, sums, hist, level8


def spread_terms(clipped, highest, lowest):
    margin = 0.01 + 0.05 * (highest - lowest)
    return highest + margin - clipped, clipped - lowest + margin


def fold(x):
    total = x[:, :LEVELS]
    for e in range(1, ELEMS):
        total = total + x[:, e * LEVELS : (e + 1) * LEVELS]
    return total


def level_sums(sums, hist, low_table, high_table):
    s = sums[:Q] + sums[Q:]
    clip = s[:, :LEVELS] + s[:, LEVELS:]
    mass = hist[0:1] + hist[1:2] + hist[2:3]

    s_low = fold(low_table * mass)
    s_high = fold(high_table * mass)
    margin = 0.01 * fold(jnp.broadcast_to(mass, (Q, mass.shape[1]))) + 0.05 * (s_high - s_low)
    return clip, s_high + margin - clip, clip - s_low + margin


def home_kernel(tracer_ref, old_ref, vals_ref, away_ref, table_ref, bt_ref, part_ref, hot_ref, peer_ref, c_ref, up_ref, down_ref, scratch, turns):
    rows = ELEMS * LEVELS
    node = iota((NODES, COLS), 0)
    column = iota((NODES, COLS), 1)
    wide = jnp.concatenate([jnp.where(column % NODES == node, jnp.broadcast_to(old_ref[e : e + 1, :], (NODES, COLS)), 0.0) for e in range(ELEMS)], axis=1)
    source_of = iota((ELEMS * COLS, rows), 0)
    gather = jnp.where(source_of // NODES == iota((ELEMS * COLS, rows), 1), 1.0, 0.0).astype(BF16)
    old = sum(dot(part, gather) for part in split3(wide))
    natural = tracer_ref[...].reshape(rows, NODES * Q)
    flat = [natural[:, 128 * j : 128 * (j + 1)].T for j in range(NODES * Q // 128)]
    for j, piece in enumerate(flat):
        table_ref[128 * j : 128 * (j + 1), :] = jnp.concatenate(split3(piece), axis=1)
    flat = jnp.concatenate(flat, axis=0)
    source = low = high = None
    for k in range(NODES):
        v = flat[k * Q : (k + 1) * Q]
        term = v * old[k : k + 1, :]
        source = term if source is None else source + term
        low = v if low is None else jnp.minimum(low, v)
        high = v if high is None else jnp.maximum(high, v)
    bt_ref[:Q] = low
    bt_ref[Q:] = high
    consts = node_constants(2 * COLS)
    table = table_ref[...]
    sums, hist = None, None
    for e in range(0, ELEMS, 2):
        args = [jnp.concatenate([vals_ref[v * ELEMS + e : v * ELEMS + e + 1], vals_ref[v * ELEMS + e + 1 : v * ELEMS + e + 2]], axis=1) for v in range(4)]
        clipped, highest, lowest, s, h, _ = evaluate(*args, table, consts)
        sums = s if sums is None else sums + s
        hist = h if hist is None else hist + h
        terms = [spread_terms(clipped[i], highest[i], lowest[i]) for i in range(Q // 8)]
        terms = (clipped, [t[0] for t in terms], [t[1] for t in terms])
        for j in range(2):
            stays = jnp.broadcast_to(away_ref[e + j : e + j + 1, :], (Q, COLS)) < 0
            for x, (term, ref) in enumerate(zip(terms, (c_ref, up_ref, down_ref))):
                v = jnp.concatenate([t[:, j * COLS : (j + 1) * COLS] for t in term], axis=0)
                v = jnp.concatenate([jnp.where(stays, v, 0.0), jnp.zeros((COLS - Q, COLS), F32)], axis=0)
                turns[x, e + j] = v.T
                for k in range(NODES):
                    at = (e + j) * COLS + LEVELS * k
                    ref[at : at + LEVELS, :] = turns[x, e + j, pl.ds(k, LEVELS, stride=NODES), :]
    clip, up, down = level_sums(sums, hist, low, high)
    pad = jnp.zeros((Q, COLS - 3 * LEVELS), F32)
    part_ref[...] = jnp.concatenate([fold(source) - clip, up, down, pad], axis=1)
    away = away_ref[...]
    hots, inside, whole = ranks(away)
    total = whole[0]
    for e in range(1, ELEMS):
        total = total + whole[e]
    device = iota((DEVS, COLS), 0)
    present = jnp.where(total > 0.0, 1.0, 0.0)
    earlier = jnp.where(iota((DEVS, COLS), 1) < device, 1.0, 0.0).astype(BF16)
    peer = dot(earlier, present.astype(BF16))
    ids = [jnp.sum(jnp.where(peer == float(p), present, 0.0) * device.astype(F32), axis=0, keepdims=True) for p in range(PEERS)]
    named = jnp.sum(present, axis=0, keepdims=True)
    ids = [ids[0]] + [jnp.where(named > float(p), ids[p], ids[0]) for p in range(1, PEERS)]
    peer_ref[...] = jnp.concatenate(ids + [named] * (8 - PEERS), axis=0).astype(I32)
    place = jnp.where(away < 0, -1.0, jnp.concatenate(spots(hots, inside, whole, peer * float(SLOTS)), axis=0))
    scratch[...] = jnp.concatenate([place, jnp.full((COLS - ELEMS, COLS), -1.0, F32)], axis=0).T
    turned = jnp.concatenate([scratch[pl.ds(k, LEVELS, stride=NODES), :] for k in range(NODES)], axis=0)
    lane = iota((COLS, SLOTS * 8), 1).astype(F32)
    for e in range(ELEMS):
        col = jnp.broadcast_to(turned[:, e : e + 1], (COLS, SLOTS * 8))
        hot_ref[e * COLS : (e + 1) * COLS, :] = jnp.where(col == lane, 1.0, 0.0).astype(BF16)


def serve_kernel(me_ref, req_ref, table_ref, part_ref, bt_ref, keep_ref, give_ref, ids_ref, level_ref, c_ref, up_ref, down_ref, dense, tiles):
    req = req_ref[...]
    sub = iota((DEVS, DEVS), 0)
    lane = iota((DEVS, DEVS), 1)
    high, mid = split2(req)
    first = jnp.where(iota((16, DEVS), 1) == 0, 1.0, 0.0).astype(BF16)
    asks = jnp.where(dot_nt(first, high) > 0.0, 1.0, 0.0)
    counter = jnp.concatenate([jnp.where(sub < lane, 1.0, 0.0).astype(BF16), jnp.ones((DEVS, DEVS), BF16)], axis=1)
    place = dot(asks.astype(BF16), counter)
    counted = place[:8, DEVS:].astype(I32)
    place = place[:, :DEVS]
    count = counted[0, 0]
    pick = jnp.where(jnp.broadcast_to(place[0:1], (DEVS, DEVS)) == sub.astype(F32), jnp.broadcast_to(asks[0:1], (DEVS, DEVS)), 0.0).astype(BF16)
    dense[...] = dot(jnp.concatenate([pick, pick], axis=1), jnp.concatenate([high, mid], axis=0))
    ids = dot_nt(iota((16, DEVS), 1).astype(F32).astype(BF16), pick)[:8].astype(I32)
    ids = jnp.where(iota((8, DEVS), 1) < counted, ids, me_ref[0])
    ids_ref[...] = jnp.where(iota((8, DEVS), 0) == 0, ids, counted)
    groups = [dense[pl.ds(i, DEVS // 4, stride=4), :] for i in range(4)]
    block = iota((DEVS // 4, DEVS), 1) // SLOTS
    for v in range(4):
        tile = None
        for i in range(4):
            shift = (i - v) * SLOTS % DEVS
            moved = pltpu.roll(groups[i], shift, 1) if shift else groups[i]
            tile = moved if tile is None else jnp.where(block == i, moved, tile)
        tiles[v] = tile
    consts = node_constants(2 * DEVS)

    def step(u, carry):
        args = [jnp.concatenate([tiles[v, pl.ds(2 * u, 1), :], tiles[v, pl.ds(2 * u + 1, 1), :]], axis=1) for v in range(4)]
        clipped, highest, lowest, s, h, level8 = evaluate(*args, table_ref[...], consts)
        for j in range(2):
            level_ref[pl.ds(pl.multiple_of(16 * u + 8 * j, 8), 8), :] = level8[:, j * DEVS : (j + 1) * DEVS]
        for i in range(Q // 8):
            up, down = spread_terms(clipped[i], highest[i], lowest[i])
            for j in range(2):
                at = pl.ds(pl.multiple_of(2 * Q * u + j * Q + 8 * i, 8), 8)
                c_ref[at, :] = clipped[i][:, j * DEVS : (j + 1) * DEVS]
                up_ref[at, :] = up[:, j * DEVS : (j + 1) * DEVS]
                down_ref[at, :] = down[:, j * DEVS : (j + 1) * DEVS]
        return carry[0] + s, carry[1] + h

    start = (jnp.zeros((2 * Q, 2 * LEVELS), F32), jnp.zeros((16, ELEMS * LEVELS), F32))
    start = step(1, step(0, start))
    sums, hist = lax.fori_loop(2, (count + 7) // 8, step, start)
    clip, up, down = level_sums(sums, hist, bt_ref[:Q, :], bt_ref[Q:, :])
    part = jnp.concatenate([-clip, up, down], axis=1) + part_ref[:, : 3 * LEVELS]
    packed = [part[8 * i : 8 * i + 8] for i in range(Q // 8)]
    packed.append(jnp.zeros((8, COLS - 3 * LEVELS * (Q // 8)), F32))
    packed = jnp.concatenate(packed, axis=1)
    upper = jnp.full((4, COLS), me_ref[0], I32) >= DEVS // 2
    keep_ref[...] = jnp.where(upper, packed[4:], packed[:4])
    give_ref[...] = jnp.where(upper, packed[:4], packed[4:])


def spread_kernel(keep_ref, got_ref, sums_ref):
    half = keep_ref[...] + got_ref[...]
    both = jnp.concatenate([half, half], axis=0)
    for d in range(DEVS // 2):
        sums_ref[8 * d : 8 * d + 8, :] = both


def finish_kernel(ids_ref, tot_ref, level_ref, c_ref, up_ref, down_ref, hc_ref, hu_ref, hd_ref, ans_ref, home_ref, later, sem):
    halves = []
    for core in range(2):
        at = core * 4 * (DEVS // 2)
        total = tot_ref[at : at + 8, :]
        for d in range(1, DEVS // 4):
            total = total + tot_ref[at + 8 * d : at + 8 * d + 8, :]
        halves.append(total[:4] + total[4:])
    total = jnp.concatenate(halves, axis=0)
    up_total = pltpu.roll(total, COLS - LEVELS, 1)
    down_total = pltpu.roll(total, COLS - 2 * LEVELS, 1)
    lanes = iota((8, COLS), 1)
    real = (lanes < 3 * LEVELS * (Q // 8)) & (lanes % (3 * LEVELS) < LEVELS)
    rise = jnp.where(real, jnp.maximum(total, 0.0) / up_total, 0.0)
    fall = jnp.where(real, jnp.minimum(total, 0.0) / down_total, 0.0)
    coef = [x[:, 24 * i : 24 * i + LEVELS] for x in (rise, fall) for i in range(Q // 8)]
    coef = jnp.concatenate(coef, axis=0)
    square = jnp.concatenate([coef, jnp.zeros((2 * Q, 128 - LEVELS), F32)], axis=1)
    turned = jnp.concatenate([square, jnp.zeros((128 - 2 * Q, 128), F32)], axis=0).T[:LEVELS]
    coef = jnp.concatenate(split3(coef), axis=1)

    def by_level(level8):
        hot = jnp.where(level8 == iota((8, 128), 0), 1.0, 0.0)
        c = dot(coef, jnp.concatenate([hot] * 3, axis=0).astype(BF16))
        return c[:Q], c[Q:]

    block = iota((CHUNK, DEVS), 1) // SLOTS

    first = ids_ref[...]

    def step(t, id_of):
        r, f = by_level(level_ref[pl.ds(pl.multiple_of(8 * t, 8), 8), :])
        at = pl.ds(pl.multiple_of(Q * t, 8), Q)
        out = c_ref[at, :] + r * up_ref[at, :] + f * down_ref[at, :]
        parts = [out[CHUNK * b : CHUNK * (b + 1)] for b in range(4)]
        for i in range(4):
            chunk = None
            for b in range(4):
                shift = (b - i) * SLOTS % DEVS
                moved = pltpu.roll(parts[b], shift, 1) if shift else parts[b]
                chunk = moved if chunk is None else jnp.where(block == b, moved, chunk)
            ans_ref[pl.ds(id_of(4 * t + i) * CHUNK, CHUNK), :] = chunk

    for t in range(3):
        step(t, lambda i: first[0, i])
    count = first[1, 0]

    @pl.when(count > 12)
    def _():
        copy = pltpu.make_async_copy(ids_ref, later, sem)
        copy.start()
        copy.wait()

        def more(t, carry):
            step(t, lambda i: later[0, i])
            return carry

        lax.fori_loop(3, (count + 3) // 4, more, 0)
    rises = jnp.concatenate([turned] * NODES, axis=0)
    falls = jnp.concatenate([pltpu.roll(turned, 128 - Q, 1)] * NODES, axis=0)
    for e in range(ELEMS):
        at = slice(e * COLS, (e + 1) * COLS)
        home_ref[at, :] = hc_ref[at, :] + rises * hu_ref[at, :] + falls * hd_ref[at, :]


def join_kernel(peer_ref, ans_ref, hot_ref, home_ref, out_hbm, out_ref, sem):
    block = iota((CHUNK, 128), 1) // SLOTS
    peers = peer_ref[...]
    chunks = [ans_ref[pl.ds(peers[p, 0] * CHUNK, CHUNK), :] for p in range(PEERS)]
    table = []
    for b in range(4):

        def moved(p):
            shift = (p - b) * SLOTS % 128
            return pltpu.roll(chunks[p], shift, 1) if shift else chunks[p]

        near = moved(0)
        for p in range(1, 4):
            near = jnp.where(block == p, moved(p), near)
        table.append(jnp.concatenate([near, jnp.where(block == 0, moved(4), 0.0)], axis=1))
    high, mid = split2(jnp.concatenate(table, axis=0))
    for e0 in range(0, ELEMS, 2):
        hot = hot_ref[e0 * COLS : (e0 + 2) * COLS, :]
        picked = dot_nt(hot, high) + dot_nt(hot, mid)
        for e in range(e0, e0 + 2):
            v = picked[(e - e0) * COLS : (e - e0 + 1) * COLS] + home_ref[e * COLS : (e + 1) * COLS, :Q]
            out_ref[e] = jnp.concatenate([v[8 * k : 8 * k + 8] for k in range(NODES)], axis=1)
            pltpu.make_async_copy(out_ref.at[e], out_hbm.at[e], sem.at[e]).start()
    for e in range(ELEMS):
        pltpu.make_async_copy(out_ref.at[e], out_hbm.at[e], sem.at[e]).wait()


def body(tracer, old_mass, new_mass, dep_owner, dep_local, dep_coord):
    me = lax.axis_index(GROUP).astype(I32).reshape(1)
    owner = dep_owner.reshape(ELEMS, COLS)
    smem, vmem, hbm = (pl.BlockSpec(memory_space=m) for m in (pltpu.SMEM, pltpu.VMEM, pltpu.HBM))

    def near(*arrays):
        return [pltpu.with_memory_space_constraint(x, pltpu.VMEM) for x in arrays]

    def call(kernel, name, outs, in_specs, scratch, args):
        return pl.pallas_call(
            kernel,
            out_shape=tuple(pltpu.VMEM(shape, dtype) for shape, dtype in outs),
            in_specs=in_specs,
            out_specs=(vmem,) * len(outs),
            scratch_shapes=scratch,
            compiler_params=pltpu.CompilerParams(vmem_limit_bytes=20 << 20),
            name=name,
        )(*args)

    def exchange(x, chunk):
        y = lax.all_to_all(x.reshape((DEVS,) + chunk), GROUP, 0, 0, tiled=True)
        return y.reshape(x.shape)

    req, away, vals, old, near_tracer = call(
        pack_kernel,
        "pack",
        (
            ((DEVS, COLS), F32),
            ((ELEMS, COLS), I32),
            ((4 * ELEMS, COLS), F32),
            ((ELEMS, COLS), F32),
            (tracer.shape, F32),
        ),
        [smem] + [hbm] * 6,
        [
            pltpu.VMEM((ELEMS, COLS), I32),
            pltpu.VMEM((ELEMS, COLS), I32),
            pltpu.VMEM((2, ELEMS, COLS), F32),
            pltpu.VMEM((ELEMS, COLS), F32),
            pltpu.SemaphoreType.DMA((6,)),
        ],
        [me] + [pltpu.with_memory_space_constraint(x, pltpu.HBM) for x in (owner, dep_local, dep_coord, new_mass, old_mass, tracer)],
    )
    asked = exchange(req, (1, COLS))
    table, bt, part, hot, peer, hc, hu, hd = call(
        home_kernel,
        "home",
        (
            ((NODES * Q, 3 * ELEMS * LEVELS), BF16),
            ((2 * Q, ELEMS * LEVELS), F32),
            ((Q, COLS), F32),
            ((ELEMS * COLS, SLOTS * 8), BF16),
            ((8, COLS), I32),
        )
        + (((ELEMS * COLS, 128), F32),) * 3,
        [vmem] * 4,
        [pltpu.VMEM((COLS, COLS), F32), pltpu.VMEM((3, ELEMS, COLS, 128), F32)],
        near(near_tracer, old, vals, away),
    )
    keep, give, ids, level, c, up, down = call(
        serve_kernel,
        "serve",
        (((4, COLS), F32), ((4, COLS), F32), ((8, DEVS), I32), ((2 * DEVS, DEVS), I32)) + (((SLOTS * Q, DEVS), F32),) * 3,
        [smem] + [vmem] * 4,
        [pltpu.VMEM((DEVS, DEVS), F32), pltpu.VMEM((4, DEVS // 4, DEVS), F32)],
        [me] + near(asked, table, part, bt),
    )
    given = lax.ppermute(give, "core", [(0, 1), (1, 0)])
    (sums,) = call(spread_kernel, "spread", (((4 * DEVS, COLS), F32),), [vmem] * 2, [], near(keep, given))
    totals = exchange(sums, (4, COLS))
    ans, home = call(
        finish_kernel,
        "finish",
        (((DEVS * CHUNK, 128), F32), ((ELEMS * COLS, 128), F32)),
        [vmem] * 9,
        [pltpu.SMEM((8, DEVS), I32), pltpu.SemaphoreType.DMA],
        near(ids, totals, level, c, up, down, hc, hu, hd),
    )
    got = exchange(ans, (1, SLOTS * Q))
    return pl.pallas_call(
        join_kernel,
        out_shape=jax.ShapeDtypeStruct((ELEMS, LEVELS, NODES * Q), F32),
        in_specs=[vmem] * 4,
        out_specs=hbm,
        scratch_shapes=[pltpu.VMEM((ELEMS, LEVELS, NODES * Q), F32), pltpu.SemaphoreType.DMA((ELEMS,))],
        compiler_params=pltpu.CompilerParams(vmem_limit_bytes=20 << 20),
        name="join",
    )(*near(peer, got, hot, home))


def solution(mesh):
    torus = Mesh(mesh.devices.reshape(4, 4, 4, 2), AXES)
    placed = (
        P(AXES, None, None),
        P(AXES, None),
        P(AXES, None),
        P(AXES, None, None),
        P(AXES, None),
        P(None, AXES, None),
    )
    return jax.shard_map(body, mesh=torus, in_specs=placed, out_specs=P(AXES, None, None), check_vma=False)
```
